512 devices in a mesh: gx: 16 (over y, core), gy: 4 (over x), gz: 8 (over z).
Axes of the slice: x: 4, y: 8, z: 8, core: 2. Of those that a mesh axis runs over, the one named last changes fastest.
Arguments:
- fractions: float32 [3, 16, 8, 16, 128], P(None, 'gx', 'gy', 'gz'), may hold values from 0 to 1
- polarizability: float32 [16, 8, 16, 128], P('gx', 'gy', 'gz'), may hold values from 0.5 to 2
- occupancy: int32 [16, 8, 16, 128], P('gx', 'gy', 'gz'), may hold values 0 or 1
- pair_mask: int32 [16, 8, 16, 27], P('gx', 'gy', 'gz'), may hold values from 0 to 1, as said below
- perm_field: float32 [6, 16, 8, 16, 128], P(None, 'gx', 'gy', 'gz'), may hold values from -6 to 6
- history: float32 [6, 6, 16, 8, 16, 128], P(None, None, 'gx', 'gy', 'gz'), may hold values from -12 to 12
Outputs:
- induced: float32 [6, 16, 8, 16, 128], P(None, 'gx', 'gy', 'gz')
- change: float32 [], replicated
The draws below stay inside these ranges and needn't reach their ends.
Inputs may be any that keep to these rules, and one draw needn't show every extreme that they name: pair_mask[t, k] equals pair_mask at tile t + offset(k) for the opposite offset 26 - k (periodic); pair_mask[t, 13] (the tile itself) is 1.
All inputs are finite; a program needn't handle non-finite values. No bound on the sum of `occupancy` on one device may be relied on, other than what follows from the above.
Results may differ from the reference program's by a relative error of at most 0.0003.
Values sent between devices are 32-bit elements; how exact they have to be, the bound alone decides.
A program may use at most 64 MiB of HBM per device.

```python
import math
import jax
import jax.numpy as jnp
from jax import lax

TILE = 128
HIST = 6
TILES_X = 1
TILES_Y = 2
TILES_Z = 2
BOX_X = 16
BOX_Y = 8
BOX_Z = 16


def draw_history(key, part):
    subkeys = jax.random.split(key, 6)
    full_shape = (6, BOX_X, BOX_Y, BOX_Z, TILE)
    block_counts = (BOX_X // TILES_X, BOX_Y // TILES_Y, BOX_Z // TILES_Z)
    frequency_table = jax.random.uniform(subkeys[4], block_counts, jnp.float32, 0.25, 2.2)
    index_x = jnp.arange(BOX_X) // TILES_X
    index_y = jnp.arange(BOX_Y) // TILES_Y
    index_z = jnp.arange(BOX_Z) // TILES_Z
    frequency = frequency_table[index_x[:, None, None], index_y[None, :, None], index_z[None, None, :]]
    step_index = jnp.arange(HIST, dtype=jnp.float32).reshape(HIST, 1, 1, 1, 1, 1)
    phase_angle = step_index * frequency[None, None, :, :, :, None]
    baseline = jax.random.normal(subkeys[0], full_shape, jnp.float32)
    cosine_part = jax.random.normal(subkeys[1], full_shape, jnp.float32)
    sine_part = jax.random.normal(subkeys[2], full_shape, jnp.float32)
    jitter = 0.2 * jax.random.normal(subkeys[3], (HIST,) + full_shape, jnp.float32)
    amplitude = jnp.exp(jax.random.uniform(subkeys[5], (1, 1, BOX_X, BOX_Y, BOX_Z, 1), jnp.float32, -0.7, 0.7))
    values = amplitude * (baseline[None] + jnp.cos(phase_angle) * cosine_part[None] + jnp.sin(phase_angle) * sine_part[None] + jitter)
    return jnp.clip(values, -12.0, 12.0).astype(jnp.float32)


def draw_pair_mask(key, part):
    coin_flips = jax.random.randint(key, (BOX_X, BOX_Y, BOX_Z, 27), 0, 4)
    one_side = (coin_flips > 0).astype(jnp.int32)
    columns = []
    for offset in range(27):
        along_x = offset // 9 - 1
        along_y = offset // 3 % 3 - 1
        along_z = offset % 3 - 1
        if offset == 13:
            columns.append(jnp.ones_like(one_side[..., offset]))
        else:
            mirror = jnp.roll(one_side[..., 26 - offset], shift=(-along_x, -along_y, -along_z), axis=(0, 1, 2))
            columns.append(one_side[..., offset] * mirror)
    return jnp.stack(columns, -1).astype(jnp.int32)


def with_ends(drawn, own_key, low, top_value):
    extent = drawn.shape
    index_at = [jax.random.randint(jax.random.fold_in(own_key, axis), (), 0, extent[axis]) for axis in range(len(extent))]
    drawn = drawn.at[tuple(index_at)].set(low)
    longest = extent.index(max(extent))
    index_at[longest] = (index_at[longest] + 1) % extent[longest]
    return drawn.at[tuple(index_at)].set(top_value)


def shard_levels(key, extent, cuts, least, high):
    loudness = 1.0
    for axis_at, blocks in cuts:
        draws = jax.random.uniform(jax.random.fold_in(jax.random.fold_in(key, 6), axis_at), (blocks,), jnp.float32, least / len(cuts), high / len(cuts))
        loudness = loudness * jnp.repeat(jnp.exp(draws), extent[axis_at] // blocks).reshape((-1,) + (1,) * (len(extent) - 1 - axis_at))
    return loudness


def scatter_about(key, dims, width, limit, pieces=(), held_as=jnp.bfloat16):
    result = jax.random.normal(key, dims, jnp.float32) * width
    if len(pieces) > 0:
        result = shard_levels(key, dims, pieces, -0.22, 0.18) * result
    return jnp.clip(result, min=-limit, max=limit).astype(held_as)


def setup_inputs(seed: int = 0) -> dict:
    key_of = jax.random.split(jax.random.key(seed), 7)
    fractions = jnp.clip(1.0 * jax.random.uniform(key_of[0], (3, BOX_X, BOX_Y, BOX_Z, TILE), jnp.float32) ** shard_levels(key_of[0], (3, BOX_X, BOX_Y, BOX_Z, TILE), ((1, 16), (2, 4), (3, 8)), -0.2, 0.2), 0.0, 1.0)
    polarizability = jnp.clip(jnp.exp(math.log(2.0) - 1.3862944 * jax.random.uniform(key_of[1], (BOX_X, BOX_Y, BOX_Z, TILE), jnp.float32) ** shard_levels(key_of[1], (BOX_X, BOX_Y, BOX_Z, TILE), ((0, 16), (1, 4), (2, 8)), -0.2, 0.2)), 0.5, 2.0)
    occupancy = with_ends((jax.random.randint(key_of[2], (BOX_X, BOX_Y, BOX_Z, TILE), 0, 8) < 7).astype(jnp.int32), jax.random.fold_in(key_of[2], 1), 0, 1)
    pair_mask = draw_pair_mask(jax.random.fold_in(key_of[6], 71), 0)
    perm_field = scatter_about(key_of[4], (6, BOX_X, BOX_Y, BOX_Z, TILE), 1.0, 6.0, ((1, 16), (2, 4), (3, 8)), jnp.float32)
    history = draw_history(jax.random.fold_in(key_of[6], 71), 0)
    return {"fractions": fractions, "polarizability": polarizability, "occupancy": occupancy, "pair_mask": pair_mask, "perm_field": perm_field, "history": history}


CELL_EDGE = 10.0
SOFTENING = 0.3
THOLE_DAMP = 0.39
RELAXATION = 0.7

def pair_field(target, source, moment, offset_vec, itself, allowed):
    displace = [(offset_vec[axis_num] + source[axis_num][:, None, :] - target[axis_num][:, :, None]) * CELL_EDGE for axis_num in range(3)]
    dist_sq = displace[0] * displace[0] + displace[1] * displace[1] + displace[2] * displace[2] + SOFTENING
    inv_cube = lax.rsqrt(dist_sq) / dist_sq
    thole_arg = dist_sq * jnp.sqrt(dist_sq) * lax.rsqrt(target[3][:, :, None] * source[3][:, None, :])
    damping = jnp.exp(-THOLE_DAMP * thole_arg)
    lambda_three = 1.0 - damping
    lambda_five = 1.0 - (1.0 + THOLE_DAMP * thole_arg) * damping
    slots = target.shape[-1]
    self_pair = jnp.logical_and(itself, jnp.eye(slots, dtype=bool))
    weight = jnp.where(self_pair, 0.0, allowed[:, None, None])
    radial = 3.0 * lambda_five * inv_cube / dist_sq * weight
    direct = lambda_three * inv_cube * weight
    fields = []
    for which_set in range(moment.shape[0] // 3):
        parts = [moment[3 * which_set + axis_num][:, None, :] for axis_num in range(3)]
        project = displace[0] * parts[0] + displace[1] * parts[1] + displace[2] * parts[2]
        for axis_num in range(3):
            fields.append(lax.optimization_barrier(jnp.sum(radial * project * displace[axis_num] - direct * parts[axis_num], axis=-1)))
    return jnp.stack(fields)

def slab_field(geometry_pad, moment_pad, allowed_slab, slab_index):
    width_y = geometry_pad.shape[2] - 2
    width_z = geometry_pad.shape[3] - 2
    slots = geometry_pad.shape[4]
    rows = moment_pad.shape[0]
    zero = jnp.zeros((), jnp.int32)
    one = jnp.ones((), jnp.int32)
    first_x = (jnp.asarray(slab_index) + 1).astype(jnp.int32)
    target = lax.dynamic_slice(geometry_pad, (zero, first_x, one, one, zero), (4, 1, width_y, width_z, slots)).reshape(4, width_y * width_z, slots)

    def offset_step(offset, summed):
        offset = jnp.asarray(offset).astype(jnp.int32)
        along_x = offset // 9 - 1
        along_y = offset // 3 % 3 - 1
        along_z = offset % 3 - 1
        starts = (zero, first_x + along_x, one + along_y, one + along_z, zero)
        source = lax.dynamic_slice(geometry_pad, starts, (4, 1, width_y, width_z, slots)).reshape(4, width_y * width_z, slots)
        moment = lax.dynamic_slice(moment_pad, starts, (rows, 1, width_y, width_z, slots)).reshape(rows, width_y * width_z, slots)
        allowed = lax.dynamic_index_in_dim(allowed_slab, offset, 2, keepdims=False).reshape(-1).astype(jnp.float32)
        offset_vec = jnp.stack([along_x, along_y, along_z]).astype(jnp.float32)
        return summed + pair_field(target, source, moment, offset_vec, offset == 13, allowed)
    summed = lax.fori_loop(0, 27, offset_step, jnp.zeros((rows, width_y * width_z, slots), jnp.float32))
    return summed.reshape(rows, width_y, width_z, slots)

def wrap_pad(values):
    return jnp.pad(values, ((0, 0), (1, 1), (1, 1), (1, 1), (0, 0)), mode='wrap')

def box_field(geometry_pad, moment, pair_mask):
    moment_pad = wrap_pad(moment)

    def one_slab(slab_index):
        allowed_slab = lax.dynamic_index_in_dim(pair_mask, slab_index, 0, keepdims=False)
        return slab_field(geometry_pad, moment_pad, allowed_slab, slab_index)
    slabs = lax.map(one_slab, jnp.arange(pair_mask.shape[0], dtype=jnp.int32))
    return jnp.moveaxis(slabs, 0, 1)

def fit_coefficients(gram_matrix):
    past_count = gram_matrix.shape[0] - 1
    gram_past = gram_matrix[:past_count, :past_count]
    gram_next = gram_matrix[:past_count, past_count]
    ridge_term = 0.001 * jnp.trace(gram_past) / past_count + 1.0
    factor = jnp.linalg.cholesky(gram_past + ridge_term * jnp.eye(past_count, dtype=jnp.float32))
    return jax.scipy.linalg.cho_solve((factor, True), gram_next)

def reference(fractions, polarizability, occupancy, pair_mask, perm_field, history):
    filled = occupancy.astype(jnp.float32)
    geometry = jnp.concatenate([fractions, polarizability[None]], 0)
    masked = history * filled
    flat_hist = masked.reshape(masked.shape[0], -1)
    gram_matrix = jnp.dot(flat_hist, flat_hist.T, precision=lax.Precision.HIGHEST)
    coeffs = fit_coefficients(gram_matrix)
    predicted = jnp.tensordot(coeffs, masked[1:], axes=1, precision=lax.Precision.HIGHEST)
    geometry_pad = wrap_pad(geometry)
    scaled = RELAXATION * filled * polarizability
    field_one = box_field(geometry_pad, predicted, pair_mask)
    dipole_one = (1.0 - RELAXATION) * predicted + scaled * (perm_field + field_one)
    field_two = box_field(geometry_pad, dipole_one, pair_mask)
    induced = (1.0 - RELAXATION) * dipole_one + scaled * (perm_field + field_two)
    update = induced - dipole_one
    change = jnp.sqrt(jnp.sum(update * update) / (jnp.sum(induced * induced) + 1.0))
    return (induced, change)
```

```python
import functools

import jax
import jax.numpy as jnp
from jax import lax
from jax.experimental import pallas as pl
from jax.experimental.pallas import tpu as pltpu
from jax.sharding import PartitionSpec as P

CELL_EDGE = 10.0
SOFTENING = 0.3
THOLE_DAMP = 0.39
RELAXATION = 0.7
MESH = pl.DeviceIdType.MESH
AXES = ("gx", "gy", "gz")
ROWS = 8
BLOCK = 32
FIELD_BLOCK = 32


def halo_moves(devices, tiles):
    options = []
    for count, n in zip(devices, tiles):
        if count == 2 and n == 2:
            around = [(1, 0, 2, 2)]
        else:
            around = [(1, n - 1, 1, n + 1), (-1, 0, 1, n)]
        options.append([(0, 0, n, 0)] + around)
    return [
        (a, b, c) for a in options[0] for b in options[1] for c in options[2] if (a[0], b[0], c[0]) != (0, 0, 0)
    ]


def row_moves(devices, tiles, row):
    along_x, along_y, along_z = [
        [(0, 0, n, 0)] + [move[axis] for move in halo_moves(devices, tiles) if move[axis][0] != 0]
        for axis, n in enumerate(tiles)
    ]
    n = tiles[1]
    rows = [(0, row, 1, row)]
    if row == n - 1:
        rows.append((1, row, 1, n + 1))
    if row == 0:
        rows.append((-1, row, 1, n))
    along_x, along_z = list(dict.fromkeys(along_x)), list(dict.fromkeys(along_z))
    return [
        (a, b, c) for a in along_x for b in rows for c in along_z if (a[0], b[0], c[0]) != (0, 0, 0)
    ]


def solve_fit(total, past, lane, pair_lane):
    def pick(a, b):
        index = pair_lane[(min(a, b), max(a, b))]
        return jnp.sum(jnp.where(lane == index, total, 0.0), axis=1, keepdims=True)

    diagonal = [pick(a, a) for a in range(past)]
    trace = diagonal[0]
    for value in diagonal[1:]:
        trace = trace + value
    ridge = 0.001 * trace / past + 1.0
    lower, inverse = {}, []
    for j in range(past):
        pivot = diagonal[j] + ridge
        for m in range(j):
            pivot = pivot - lower[j, m] * lower[j, m]
        inverse.append(1.0 / jnp.sqrt(pivot))
        for i in range(j + 1, past):
            value = pick(i, j)
            for m in range(j):
                value = value - lower[i, m] * lower[j, m]
            lower[i, j] = value * inverse[j]
    forward = []
    for i in range(past):
        value = pick(i, past)
        for m in range(i):
            value = value - lower[i, m] * forward[m]
        forward.append(value * inverse[i])
    coeffs = [None] * past
    for i in reversed(range(past)):
        value = forward[i]
        for m in range(i + 1, past):
            value = value - lower[m, i] * coeffs[m]
        coeffs[i] = value * inverse[i]
    return coeffs


def kernel(
    devices,
    frac_in, pol_in, occ_in, mask_in, perm_in, hist_in,
    out_ref, change_ref,
    frac_ref, pol_ref, occ_ref, mask_ref, perm_ref, hist_ref,
    geom, held_one, held_two, past_sets, own, apart, pull, direct, sums, slots_a, slots_b, slots_c, slots_d,
    load_sem, send_all, recv_all, send_geom, recv_geom, send_one, recv_one, send_two, recv_two,
):
    tiles = tuple(frac_ref.shape[1:4])
    slots = frac_ref.shape[4]
    steps = hist_ref.shape[0]
    rows = hist_ref.shape[1]
    past = steps - 1
    at = [lax.axis_index(axis) for axis in AXES]
    moves = halo_moves(devices, tiles)
    lane = lax.broadcasted_iota(jnp.int32, (1, slots), 1)
    loads = [
        pltpu.make_async_copy(source, target, load_sem.at[number])
        for number, (source, target) in enumerate(
            (
                (hist_in, hist_ref), (occ_in, occ_ref), (frac_in, frac_ref),
                (pol_in, pol_ref), (perm_in, perm_ref), (mask_in, mask_ref),
            )
        )
    ]
    for load in loads:
        load.start()

    groups = ((0,), (1, 2))

    def size_of(axes):
        total = 1
        for axis in axes:
            total *= devices[axis]
        return total

    def shifted(shift):
        places = []
        for axis in range(3):
            place = at[axis] + shift[axis]
            places.append(jnp.where(place >= devices[axis], place - devices[axis], place))
        return tuple(places)

    def hops(shift):
        return sum(min(part, n - part) for part, n in zip(shift, devices))

    def shifts_of(axes):
        spans = [range(devices[axis]) if axis in axes else range(1) for axis in range(3)]
        every = [(x, y, z) for x in spans[0] for y in spans[1] for z in spans[2] if (x, y, z) != (0, 0, 0)]
        return sorted(every, key=lambda shift: -hops(shift))

    def rank_in(axes):
        rank = 0
        for axis in axes:
            rank = rank * devices[axis] + at[axis]
        return rank

    near = [tuple((move[axis][0] + devices[axis]) % devices[axis] for axis in range(3)) for move in moves]
    greeted = list(dict.fromkeys([shift for axes in groups for shift in shifts_of(axes)] + near))

    barrier = pltpu.get_barrier_semaphore()

    for shift in greeted:
        pl.semaphore_signal(barrier, inc=1, device_id=shifted(shift), device_id_type=MESH)
    for load in loads:
        load.wait()

    def share(index, stage, held, value):
        axes = groups[stage]
        rank = rank_in(axes)
        held[pl.ds(rank, 1)] = value.reshape(1, 1, slots)
        for shift in shifts_of(axes):
            pltpu.make_async_remote_copy(
                src_ref=held.at[pl.ds(rank, 1)],
                dst_ref=held.at[pl.ds(rank, 1)],
                send_sem=send_all.at[index, stage],
                recv_sem=recv_all.at[index, stage],
                device_id=shifted(shift),
                device_id_type=MESH,
            ).start()

    def collect(index, stage, held):
        others = size_of(groups[stage]) - 1
        whole = pltpu.make_async_remote_copy(
            src_ref=held.at[pl.ds(0, others)],
            dst_ref=held.at[pl.ds(0, others)],
            send_sem=send_all.at[index, stage],
            recv_sem=recv_all.at[index, stage],
            device_id=shifted((0, 0, 1)),
            device_id_type=MESH,
        )
        whole.wait_send()
        whole.wait_recv()
        return jnp.sum(held[...], axis=0)

    def halo(held, send, recv, moves=moves):
        copies = []
        for number, move in enumerate(moves):
            source = tuple(pl.ds(part[1], part[2]) for part in move)
            place = tuple(pl.ds(part[3], part[2]) for part in move)
            target = tuple((at[axis] + move[axis][0] + devices[axis]) % devices[axis] for axis in range(3))
            copies.append(
                pltpu.make_async_remote_copy(
                    src_ref=held.at[source],
                    dst_ref=held.at[place],
                    send_sem=send.at[number],
                    recv_sem=recv.at[number],
                    device_id=target,
                    device_id_type=MESH,
                )
            )
        return copies

    places = [(x, y, z) for x in range(tiles[0]) for y in range(tiles[1]) for z in range(tiles[2])]
    zero_row = jnp.zeros((1, slots), jnp.float32)
    spare = jnp.zeros((ROWS - rows, slots), jnp.float32)
    filled, scaled, fixed = [], [], []
    for t, (x, y, z) in enumerate(places):
        full = occ_ref[x, y, z, :].reshape(1, slots).astype(jnp.float32)
        pol = pol_ref[x, y, z, :].reshape(1, slots)
        scaled.append(RELAXATION * full * pol)
        tile = jnp.concatenate(
            [frac_ref[c, x, y, z, :].reshape(1, slots) * CELL_EDGE for c in range(3)]
            + [lax.rsqrt(pol)] + [zero_row] * (ROWS - 4),
            axis=0,
        )
        geom[x, y, z] = tile
        for h in range(steps):
            moment = jnp.concatenate(
                [hist_ref[h, c, x, y, z, :].reshape(1, slots) for c in range(rows)], axis=0
            )
            past_sets[h, t] = jnp.concatenate([moment * full, spare], axis=0)
        fixed.append(
            jnp.concatenate(
                [perm_ref[c, x, y, z, :].reshape(1, slots) for c in range(rows)] + [spare], axis=0
            )
        )
    pair_lane = {}
    gram = zero_row
    for a in range(steps):
        for b in range(a, steps):
            product = past_sets[a, 0] * past_sets[b, 0]
            for t in range(1, len(places)):
                product = product + past_sets[a, t] * past_sets[b, t]
            value = jnp.sum(jnp.sum(product, axis=0, keepdims=True), axis=1, keepdims=True)
            pair_lane[(a, b)] = len(pair_lane)
            gram = jnp.where(lane == pair_lane[(a, b)], value, gram)

    for t, (x, y, z) in enumerate(places):
        for c in range(4):
            row = geom[x, y, z, c, :].reshape(1, slots)
            own[t, c] = jnp.broadcast_to(row, (slots, slots)).T

    pl.semaphore_wait(barrier, len(greeted))
    geom_copies = halo(geom, send_geom, recv_geom)
    share(0, 0, slots_a, gram)
    for copy in geom_copies:
        copy.start()

    def clear(step, carry):
        sums[step] = jnp.zeros((rows, slots, slots), jnp.float32)
        return carry

    lax.fori_loop(0, 2 * len(places), clear, 0)
    for move, copy in zip(moves, geom_copies):
        if move[0][0] == 0:
            copy.wait()

    wraps = tuple(n + 2 for n in tiles)

    def wrap(value, size):
        return jnp.where(value < 0, value + size, value)

    def spot(t):
        x = t // (tiles[1] * tiles[2])
        y = t // tiles[2] % tiles[1]
        z = t % tiles[2]
        return (x, y, z)

    def source_rows(held, place, names):
        return [held[place[0], place[1], place[2], pl.ds(c, 1), :] for c in names]

    def geometry(t, nine):
        along_x, along_y = nine // 3 - 1, nine % 3 - 1
        base = spot(t)
        for along_z in (-1, 0, 1):
            along = (along_x, along_y, along_z)
            k = nine * 3 + along_z + 1
            place = tuple(wrap(base[i] + along[i], wraps[i]) for i in range(3))
            source = source_rows(geom, place, range(4))
            source[0] = source[0] + CELL_EDGE * along_x.astype(jnp.float32)
            source[1] = source[1] + CELL_EDGE * along_y.astype(jnp.float32)
            source[2] = source[2] + CELL_EDGE * along_z
            damp = source[3] * THOLE_DAMP
            allowed = mask_ref[base[0], base[1], base[2], k].astype(jnp.float32)
            for first in range(0, slots, BLOCK):
                part = pl.ds(first, BLOCK)
                dx = source[0] - own[t, 0, part, :]
                dy = source[1] - own[t, 1, part, :]
                dz = source[2] - own[t, 2, part, :]
                square = dx * dx + dy * dy + dz * dz + SOFTENING
                root = lax.rsqrt(square)
                root_two = root * root
                cube = root_two * root * allowed
                arg = (square * square) * root * (damp * own[t, 3, part, :])
                fade = jnp.exp(-arg)
                three = 1.0 - fade
                five = three - arg * fade
                direct[t, k, part, :] = three * cube
                radial = five * cube * (3.0 * root_two)
                for i, d in enumerate((dx, dy, dz)):
                    apart[i, t, k, part, :] = d
                    pull[i, t, k, part, :] = radial * d

    count = len(places)

    def same_x(step, carry):
        geometry(step // 3, 3 + step % 3)
        return carry

    def other_x(step, carry):
        part = step % 6
        geometry(step // 6, jnp.where(part < 3, part, part + 3))
        return carry

    lax.fori_loop(0, count * 2, same_x, 0)
    share(0, 1, slots_b, collect(0, 0, slots_a))
    lax.fori_loop(count * 2, count * 3, same_x, 0)
    total = collect(0, 1, slots_b)
    coeffs = solve_fit(total, past, lane, pair_lane)
    for t, (x, y, z) in enumerate(places):
        value = coeffs[0] * past_sets[1, t]
        for h in range(1, past):
            value = value + coeffs[h] * past_sets[h + 1, t]
        held_one[x, y, z] = value
    one_copies = halo(held_one, send_one, recv_one)
    for copy in one_copies:
        copy.start()
    for move, copy in zip(moves, geom_copies):
        if move[0][0] != 0:
            copy.wait()
    lax.fori_loop(0, count * 6, other_x, 0)
    off_diagonal = lax.broadcasted_iota(jnp.int32, (slots, slots), 0) != lax.broadcasted_iota(
        jnp.int32, (slots, slots), 1
    )
    for t in range(count):
        direct[t, 13] = jnp.where(off_diagonal, direct[t, 13], 0.0)

    blocks = slots // FIELD_BLOCK

    def add_sources(held, index, step, base, along_y):
        part = pl.ds(pl.multiple_of(step % blocks * FIELD_BLOCK, FIELD_BLOCK), FIELD_BLOCK)
        t = (base[0] * tiles[1] + base[1]) * tiles[2] + base[2]
        place_y = wrap(base[1] + along_y, wraps[1])

        def plane(along_x, acc):
            acc = list(acc)
            place_x = wrap(base[0] + along_x, wraps[0])
            for along_z in (-1, 0, 1):
                place = (place_x, place_y, wrap(base[2] + along_z, wraps[2]))
                moment = source_rows(held, place, range(rows))
                k = 9 * (along_x + 1) + 3 * (along_y + 1) + along_z + 1
                d = direct[t, k, part, :]
                away = [apart[i, t, k, part, :] for i in range(3)]
                drawn = [pull[i, t, k, part, :] for i in range(3)]
                for s in range(rows // 3):
                    m = moment[3 * s : 3 * s + 3]
                    project = away[0] * m[0] + away[1] * m[1] + away[2] * m[2]
                    for i in range(3):
                        acc[3 * s + i] = acc[3 * s + i] + (project * drawn[i] - d * m[i])
            return tuple(acc)

        acc = lax.fori_loop(
            -1, 2, plane, tuple(sums[index * count + t, c, part, :] for c in range(rows))
        )
        for c in range(rows):
            sums[index * count + t, c, part, :] = acc[c]

    flat = tiles[0] * tiles[2] * blocks

    def to_row(held, index, row):
        def one(step, carry):
            column = step // blocks % (tiles[0] * tiles[2])
            base = (column // tiles[2], row, column % tiles[2])
            add_sources(held, index, step, base, step // flat - 1)
            return carry

        lax.fori_loop(0, 3 * flat, one, 0)

    def from_row(held, index, row):
        def one(step, carry):
            column = step // blocks % (tiles[0] * tiles[2])
            along_y = step // flat - 1
            base = (column // tiles[2], (row - along_y + tiles[1]) % tiles[1], column % tiles[2])
            add_sources(held, index, step, base, along_y)
            return carry

        lax.fori_loop(0, 3 * flat, one, 0)

    square_lane = lax.broadcasted_iota(jnp.int32, (slots, slots), 1)

    def field_of(index, t):
        columns = jnp.zeros((slots, slots), jnp.float32)
        for c in range(rows):
            value = jnp.sum(sums[index * count + t, c], axis=1, keepdims=True)
            columns = jnp.where(square_lane == c, value, columns)
        return columns.T[0:ROWS]

    for copy in one_copies:
        copy.wait()
    two_copies = []
    for row in range(tiles[1]):
        to_row(held_one, 0, row)
        for t, (x, y, z) in enumerate(places):
            if y == row:
                held_two[x, y, z] = (1.0 - RELAXATION) * held_one[x, y, z] + scaled[t] * (
                    fixed[t] + field_of(0, t)
                )
        copies = halo(held_two, send_two.at[row], recv_two.at[row], row_moves(devices, tiles, row))
        for copy in copies:
            copy.start()
        two_copies.append(copies)
    for row in range(tiles[1]):
        for copy in two_copies[row]:
            copy.wait()
        from_row(held_two, 1, row)
    fields = [field_of(1, t) for t in range(count)]
    changed = jnp.zeros((ROWS, slots), jnp.float32)
    size = jnp.zeros((ROWS, slots), jnp.float32)
    for t, (x, y, z) in enumerate(places):
        before = held_two[x, y, z]
        after = (1.0 - RELAXATION) * before + scaled[t] * (fixed[t] + fields[t])
        for c in range(rows):
            out_ref[c, x, y, z, :] = after[c]
        changed = changed + (after - before) * (after - before)
        size = size + after * after

    def all_of(value):
        return jnp.sum(jnp.sum(value, axis=0, keepdims=True), axis=1, keepdims=True)

    pair = jnp.where(lane == 0, all_of(changed), jnp.where(lane == 1, all_of(size), 0.0))
    share(1, 0, slots_c, pair)
    share(1, 1, slots_d, collect(1, 0, slots_c))
    pair = collect(1, 1, slots_d)
    above = jnp.sum(jnp.where(lane == 0, pair, 0.0), axis=1, keepdims=True)
    below = jnp.sum(jnp.where(lane == 1, pair, 0.0), axis=1, keepdims=True)
    change_ref[...] = jnp.broadcast_to(jnp.sqrt(above / (below + 1.0)), (1, slots))


def solution(mesh):
    devices = tuple(mesh.shape[axis] for axis in AXES)

    def on_device(fractions, polarizability, occupancy, pair_mask, perm_field, history):
        tiles = fractions.shape[1:4]
        slots = fractions.shape[4]
        count = tiles[0] * tiles[1] * tiles[2]
        wraps = tuple(n + 2 for n in tiles)
        moves = len(halo_moves(devices, tiles))
        rows = history.shape[1]
        vmem = pl.BlockSpec(memory_space=pltpu.VMEM)
        f32 = jnp.float32
        induced, change = pl.pallas_call(
            functools.partial(kernel, devices),
            out_shape=(
                jax.ShapeDtypeStruct(perm_field.shape, f32),
                jax.ShapeDtypeStruct((1, slots), f32),
            ),
            in_specs=[pl.BlockSpec(memory_space=pltpu.HBM)] * 6,
            out_specs=(vmem, vmem),
            scratch_shapes=[
                pltpu.VMEM(fractions.shape, f32),
                pltpu.VMEM(polarizability.shape, f32),
                pltpu.VMEM(occupancy.shape, jnp.int32),
                pltpu.SMEM(pair_mask.shape, jnp.int32),
                pltpu.VMEM(perm_field.shape, f32),
                pltpu.VMEM(history.shape, f32),
                pltpu.VMEM(wraps + (ROWS, slots), f32),
                pltpu.VMEM(wraps + (ROWS, slots), f32),
                pltpu.VMEM(wraps + (ROWS, slots), f32),
                pltpu.VMEM((history.shape[0], count, ROWS, slots), f32),
                pltpu.VMEM((count, 4, slots, slots), f32),
                pltpu.VMEM((3, count, 27, slots, slots), f32),
                pltpu.VMEM((3, count, 27, slots, slots), f32),
                pltpu.VMEM((count, 27, slots, slots), f32),
                pltpu.VMEM((2 * count, rows, slots, slots), f32),
                pltpu.VMEM((devices[0], 1, slots), f32),
                pltpu.VMEM((devices[1] * devices[2], 1, slots), f32),
                pltpu.VMEM((devices[0], 1, slots), f32),
                pltpu.VMEM((devices[1] * devices[2], 1, slots), f32),
                pltpu.SemaphoreType.DMA((6,)),
                pltpu.SemaphoreType.DMA((2, 2)),
                pltpu.SemaphoreType.DMA((2, 2)),
            ]
            + [pltpu.SemaphoreType.DMA((moves,))] * 4
            + [pltpu.SemaphoreType.DMA((tiles[1], moves))] * 2,
            compiler_params=pltpu.CompilerParams(
                collective_id=0, has_side_effects=True, vmem_limit_bytes=67043328
            ),
        )(fractions, polarizability, occupancy, pair_mask, perm_field, history)
        return induced, change[0, 0]

    in_specs = (
        P(None, "gx", "gy", "gz", None),
        P("gx", "gy", "gz", None),
        P("gx", "gy", "gz", None),
        P("gx", "gy", "gz", None),
        P(None, "gx", "gy", "gz", None),
        P(None, None, "gx", "gy", "gz", None),
    )
    out_specs = (P(None, "gx", "gy", "gz", None), P())
    return jax.shard_map(
        on_device, mesh=mesh, in_specs=in_specs, out_specs=out_specs, check_vma=False
    )
```

```python
import functools

import jax
import jax.numpy as jnp
from jax import lax
from jax.experimental import pallas as pl
from jax.experimental.pallas import tpu as pltpu
from jax.sharding import PartitionSpec as P

CELL_EDGE = 10.0
SOFTENING = 0.3
THOLE_DAMP = 0.39
RELAXATION = 0.7
LOG2E = 1.4426950408889634
MESH = pl.DeviceIdType.MESH
AXES = ("gx", "gy", "gz")
ROWS = 8
BLOCK = 32
GROUPS = ((0,), (1, 2))


def halo_moves(tiles):
    options = []
    for n in tiles:
        options.append([(0, 0, n, 0), (1, n - 1, 1, n + 1), (-1, 0, 1, n)])
    return [
        (a, b, c) for a in options[0] for b in options[1] for c in options[2] if (a[0], b[0], c[0]) != (0, 0, 0)
    ]


def solve_fit(total, past, lane, pair_lane):
    def pick(a, b):
        index = pair_lane[(min(a, b), max(a, b))]
        return jnp.sum(jnp.where(lane == index, total, 0.0), axis=1, keepdims=True)

    diagonal = [pick(a, a) for a in range(past)]
    trace = diagonal[0]
    for value in diagonal[1:]:
        trace = trace + value
    ridge = 0.001 * trace / past + 1.0
    lower, inverse = {}, []
    for j in range(past):
        pivot = diagonal[j] + ridge
        for m in range(j):
            pivot = pivot - lower[j, m] * lower[j, m]
        inverse.append(lax.rsqrt(pivot))
        for i in range(j + 1, past):
            value = pick(i, j)
            for m in range(j):
                value = value - lower[i, m] * lower[j, m]
            lower[i, j] = value * inverse[j]
    forward = []
    for i in range(past):
        value = pick(i, past)
        for m in range(i):
            value = value - lower[i, m] * forward[m]
        forward.append(value * inverse[i])
    coeffs = [None] * past
    for i in reversed(range(past)):
        value = forward[i]
        for m in range(i + 1, past):
            value = value - lower[m, i] * coeffs[m]
        coeffs[i] = value * inverse[i]
    return coeffs


def kernel(
    devices,
    frac_in, pol_in, occ_in, mask_in, perm_in, hist_in,
    out_ref, change_ref,
    frac_ref, pol_ref, occ_ref, mask_ref, perm_ref, hist_ref,
    geom, held_past, held_two, past_sets, spots, columns, features, weights,
    slots_a, slots_b, slots_c, slots_d,
    load_sem, send_all, recv_all, send_geom, recv_geom, send_past, recv_past, send_two, recv_two,
):
    tiles = tuple(frac_ref.shape[1:4])
    wraps = tuple(n + 2 for n in tiles)
    slots = frac_ref.shape[4]
    steps = hist_ref.shape[0]
    rows = hist_ref.shape[1]
    past = steps - 1
    at = [lax.axis_index(axis) for axis in AXES]
    moves = halo_moves(tiles)
    lane = lax.broadcasted_iota(jnp.int32, (1, slots), 1)
    loads = [
        pltpu.make_async_copy(source, target, load_sem.at[number])
        for number, (source, target) in enumerate(
            (
                (hist_in, hist_ref), (occ_in, occ_ref), (frac_in, frac_ref),
                (pol_in, pol_ref), (perm_in, perm_ref), (mask_in, mask_ref),
            )
        )
    ]
    for load in loads:
        load.start()

    def size_of(axes):
        total = 1
        for axis in axes:
            total *= devices[axis]
        return total

    def shifted(shift):
        places = []
        for axis in range(3):
            place = at[axis] + shift[axis]
            places.append(jnp.where(place >= devices[axis], place - devices[axis], place))
        return tuple(places)

    def hops(shift):
        return sum(min(part, n - part) for part, n in zip(shift, devices))

    def shifts_of(axes):
        spans = [range(devices[axis]) if axis in axes else range(1) for axis in range(3)]
        every = [(x, y, z) for x in spans[0] for y in spans[1] for z in spans[2] if (x, y, z) != (0, 0, 0)]
        return sorted(every, key=lambda shift: -hops(shift))

    def rank_in(axes):
        rank = 0
        for axis in axes:
            rank = rank * devices[axis] + at[axis]
        return rank

    near = [tuple((move[axis][0] + devices[axis]) % devices[axis] for axis in range(3)) for move in moves]
    greeted = list(dict.fromkeys([shift for axes in GROUPS for shift in shifts_of(axes)] + near))

    barrier = pltpu.get_barrier_semaphore()

    for shift in greeted:
        pl.semaphore_signal(barrier, inc=1, device_id=shifted(shift), device_id_type=MESH)
    for load in loads:
        load.wait()

    def share(index, stage, held, value):
        axes = GROUPS[stage]
        rank = rank_in(axes)
        held[pl.ds(rank, 1)] = value.reshape(1, 1, slots)
        for shift in shifts_of(axes):
            pltpu.make_async_remote_copy(
                src_ref=held.at[pl.ds(rank, 1)],
                dst_ref=held.at[pl.ds(rank, 1)],
                send_sem=send_all.at[index, stage],
                recv_sem=recv_all.at[index, stage],
                device_id=shifted(shift),
                device_id_type=MESH,
            ).start()

    def collect(index, stage, held):
        others = size_of(GROUPS[stage]) - 1
        whole = pltpu.make_async_remote_copy(
            src_ref=held.at[pl.ds(0, others)],
            dst_ref=held.at[pl.ds(0, others)],
            send_sem=send_all.at[index, stage],
            recv_sem=recv_all.at[index, stage],
            device_id=shifted((0, 0, 1)),
            device_id_type=MESH,
        )
        whole.wait_send()
        whole.wait_recv()
        return jnp.sum(held[...], axis=0)

    def halo(held, send, recv):
        copies = []
        for number, move in enumerate(moves):
            source = tuple(pl.ds(part[1], part[2]) for part in move)
            place = tuple(pl.ds(part[3], part[2]) for part in move)
            copies.append(
                pltpu.make_async_remote_copy(
                    src_ref=held.at[source],
                    dst_ref=held.at[place],
                    send_sem=send.at[number],
                    recv_sem=recv.at[number],
                    device_id=shifted(near[number]),
                    device_id_type=MESH,
                )
            )
        return copies

    def row_of(c):
        return 2 * (c % 3) + c // 3

    order = sorted(range(rows), key=row_of)
    places = [(x, y, z) for x in range(tiles[0]) for y in range(tiles[1]) for z in range(tiles[2])]
    count = len(places)
    zero_row = jnp.zeros((1, slots), jnp.float32)
    spare = jnp.zeros((ROWS - rows, slots), jnp.float32)
    scaled = []
    for t, (x, y, z) in enumerate(places):
        full = occ_ref[x, y, z, :].reshape(1, slots).astype(jnp.float32)
        pol = pol_ref[x, y, z, :].reshape(1, slots)
        scaled.append(RELAXATION * full * pol)
        parts = []
        for c in range(3):
            parts += [frac_ref[c, x, y, z, :].reshape(1, slots) * CELL_EDGE] * 2
        geom[x, y, z] = jnp.concatenate(parts + [lax.rsqrt(pol), zero_row], axis=0)
        for h in range(steps):
            moment = jnp.concatenate(
                [hist_ref[h, c, x, y, z, :].reshape(1, slots) for c in order] + [spare], axis=0
            ) * full
            past_sets[h, t] = moment
            if h > 0:
                held_past[x, y, z, pl.ds(ROWS * (h - 1), ROWS), :] = moment
    pair_lane = {}
    gram = zero_row
    for a in range(steps):
        for b in range(a, steps):
            product = past_sets[a, 0] * past_sets[b, 0]
            for t in range(1, count):
                product = product + past_sets[a, t] * past_sets[b, t]
            value = jnp.sum(jnp.sum(product, axis=0, keepdims=True), axis=1, keepdims=True)
            pair_lane[(a, b)] = len(pair_lane)
            gram = jnp.where(lane == pair_lane[(a, b)], value, gram)

    row = lax.broadcasted_iota(jnp.int32, (ROWS, slots), 0)
    wide_row = lax.broadcasted_iota(jnp.int32, (ROWS, 2 * slots), 0)

    square_row = lax.broadcasted_iota(jnp.int32, (slots, slots), 0)
    square_lane = lax.broadcasted_iota(jnp.int32, (slots, slots), 1)

    def flat_of(place):
        return (place[0] * wraps[1] + place[1]) * wraps[2] + place[2]

    def wrap(value, size):
        return jnp.where(value < 0, value + size, value)

    def prepare(place):
        flat = flat_of(place)
        tile = geom[place[0], place[1], place[2]]
        moved = []
        for axis in range(3):
            number = jnp.where(place[axis] == wraps[axis] - 1, -1, place[axis])
            moved.append(CELL_EDGE * (number.astype(jnp.float32) - 0.5 * tiles[axis]))
        offset = jnp.where(row < 2, moved[0], jnp.where(row < 4, moved[1], jnp.where(row < 6, moved[2], 0.0)))
        tile = tile + offset
        spots[flat] = tile
        upright = tile.T
        for c in range(4):
            columns[flat, c] = jnp.broadcast_to(upright[:, 2 * c : 2 * c + 1], (slots, slots))

    def split(t):
        return lax.shift_right_logical(t, 1), lax.bitwise_and(t, 1)

    def pair_weights(t, along, itself):
        first_y, first_z = split(t)
        base = (jnp.int32(0), first_y, first_z)
        place = tuple(wrap(base[i] + along[i], wraps[i]) for i in range(3))
        k = 9 * (along[0] + 1) + 3 * (along[1] + 1) + along[2] + 1
        source = flat_of(place)
        own = flat_of(base)
        here = [spots[own, pl.ds(2 * c, 1), :] for c in range(4)]
        allowed = mask_ref[0, first_y, first_z, k].astype(jnp.float32)
        damp = here[3] * (-THOLE_DAMP * allowed)
        for first in range(0, slots, BLOCK):
            part = pl.ds(first, BLOCK)
            dx = columns[source, 0, part, :] - here[0]
            dy = columns[source, 1, part, :] - here[1]
            dz = columns[source, 2, part, :] - here[2]
            square = dx * dx + dy * dy + (dz * dz + SOFTENING)
            root = lax.rsqrt(square)
            root_two = root * root
            cube = root_two * root
            arg = (square * square) * root * (damp * columns[source, 3, part, :])
            fade = jnp.exp2(arg * LOG2E)
            three = 1.0 - fade
            five = three + arg * fade
            radial, direct = five * cube * root_two, three * cube
            if itself:
                apart = square_row[first : first + BLOCK] != square_lane[first : first + BLOCK]
                radial, direct = jnp.where(apart, radial, 0.0), jnp.where(apart, direct, 0.0)
            both = jnp.concatenate([radial, direct], axis=1)
            high = both.astype(jnp.bfloat16)
            weights[t, k, part, :] = high
            weights[t, k, pl.ds(slots + first, BLOCK), :] = (both - high.astype(jnp.float32)).astype(jnp.bfloat16)

    def outward(t):
        first_y, first_z = split(t)
        return 2 * first_y - 1, 2 * first_z - 1

    def inner_pairs(t, carry):
        out_y, out_z = outward(t)
        for q in range(4):
            pair_weights(t, (0, -out_y * (q // 2), -out_z * (q % 2)), q == 0)
        return carry

    def edge_pairs(t, carry):
        out_y, out_z = outward(t)
        for along in ((out_y, -1), (out_y, 0), (out_y, 1), (0, out_z), (-out_y, out_z)):
            pair_weights(t, (0,) + along, False)
        return carry

    def plane_pairs(along_x):
        def one(t, carry):
            for q in range(9):
                pair_weights(t, (along_x, q // 3 - 1, q % 3 - 1), False)
            return carry

        return one

    for place in places:
        prepare(tuple(jnp.int32(part) for part in place))
    lax.fori_loop(0, count, inner_pairs, 0)

    pl.semaphore_wait(barrier, len(greeted))
    share(0, 0, slots_a, gram)
    geom_copies = halo(geom, send_geom, recv_geom)
    for copy in geom_copies:
        copy.start()
    past_copies = halo(held_past, send_past, recv_past)
    for copy in past_copies:
        copy.start()
    for copy in geom_copies:
        copy.wait()

    for y in range(wraps[1]):
        for z in range(wraps[2]):
            if y >= tiles[1] or z >= tiles[2]:
                prepare((jnp.int32(0), jnp.int32(y), jnp.int32(z)))

    def prepare_eight(step, carry):
        half_x, half_y = split(step)
        for q in range(8):
            prepare((1 + half_x, 2 * half_y + q // 4, jnp.int32(q % 4)))
        return carry

    lax.fori_loop(0, 4, prepare_eight, 0)
    share(0, 1, slots_b, collect(0, 0, slots_a))
    lax.fori_loop(0, count, edge_pairs, 0)
    lax.fori_loop(0, count, plane_pairs(-1), 0)
    lax.fori_loop(0, count, plane_pairs(1), 0)

    def cycle(value):
        value = value + pltpu.roll(value, 4, 0)
        return value + pltpu.roll(value, 2, 0)

    def rounded(value):
        return value.astype(jnp.bfloat16).astype(jnp.float32)

    def set_features(pair, moment):
        twice = [2 * pair, 2 * pair + 1]
        spot = jnp.concatenate([spots[flat] for flat in twice], axis=1)
        spot = jnp.where(wide_row < rows, spot, 0.0)
        by = [
            jnp.concatenate([spots[flat, pl.ds(2 * c, 1), :] for flat in twice], axis=1) * moment
            for c in range(3)
        ]
        first = jnp.concatenate([moment, by[0]], axis=0)
        second = jnp.concatenate(by[1:], axis=0)
        third = cycle(spot * moment) * spot
        middle = third - rounded(third)
        last = middle - rounded(middle)
        blocks = []
        for piece in range(3):
            blocks += [first, second]
            if piece < 2:
                first = first - rounded(first)
                second = second - rounded(second)
        blocks.append(jnp.concatenate([third, middle], axis=0))
        blocks.append(jnp.concatenate([last, jnp.zeros_like(last)], axis=0))
        for number, value in enumerate(blocks):
            features[pair, pl.ds(2 * ROWS * number, 2 * ROWS), :] = value.astype(jnp.bfloat16)

    def along_of(k):
        return (k // 9 - 1, k // 3 % 3 - 1, k % 3 - 1)

    def target_of(place, k):
        along = along_of(k)
        return tuple((place[i] + along[i] + wraps[i]) % wraps[i] for i in range(3))

    def distance(place):
        return sum(part >= n for part, n in zip(place, tiles))

    def partial_sums(t, chosen):
        acc = None
        for k in range(27):
            place = target_of(places[t], k)
            if distance(place) in chosen:
                flat = flat_of(place)
                side = features[flat // 2, :, pl.ds(flat % 2 * slots, slots)]
                part = jnp.dot(
                    jnp.concatenate([side, side], axis=1), weights[t, k], preferred_element_type=jnp.float32
                )
                acc = part if acc is None else acc + part
        group = [acc[ROWS * g : ROWS * (g + 1)] for g in range(2 * ROWS)]
        sums = [(group[8 + g] + group[4 + g] + group[g])[:, 0:slots] for g in range(4)]
        sums.append((group[14] + group[13] + group[12])[:, 0:slots])
        sums.append((group[8] + group[4] + group[0])[:, slots : 2 * slots])
        return sums

    def field_of(t, sums):
        plain, by_x, by_y, by_z, whole, direct = sums
        spot = jnp.where(row < rows, spots[flat_of(places[t])], 0.0)
        mine = [cycle(spot * value) for value in (by_x, by_y, by_z)]
        middle = jnp.where(row < 2, by_x, jnp.where(row < 4, by_y, by_z))
        drawn = jnp.where(row < 2, mine[0], jnp.where(row < 4, mine[1], mine[2]))
        radial = whole - drawn + spot * cycle(spot * plain - middle)
        return jnp.where(row < rows, 3.0 * radial - direct, 0.0)

    fixed = [
        jnp.concatenate([perm_ref[c, x, y, z, :].reshape(1, slots) for c in order] + [spare], axis=0)
        for (x, y, z) in places
    ]
    for copy in past_copies:
        copy.wait()
    total = collect(0, 1, slots_b)
    coeffs = [jnp.broadcast_to(value, (ROWS, slots)) for value in solve_fit(total, past, lane, pair_lane)]

    def predicted(x, y, z):
        value = coeffs[0] * held_past[x, y, z, pl.ds(0, ROWS), :]
        for h in range(1, past):
            value = value + coeffs[h] * held_past[x, y, z, pl.ds(ROWS * h, ROWS), :]
        return value

    def predict(step, carry):
        x, y = lax.shift_right_logical(step, 2), lax.bitwise_and(step, 3)
        for half in range(2):
            moment = jnp.concatenate([predicted(x, y, 2 * half), predicted(x, y, 2 * half + 1)], axis=1)
            set_features(2 * step + half, moment)
        return carry

    lax.fori_loop(0, wraps[0] * wraps[1], predict, 0)
    ones = []
    for t, (x, y, z) in enumerate(places):
        field = field_of(t, partial_sums(t, (0, 1, 2, 3)))
        value = (1.0 - RELAXATION) * predicted(x, y, z) + scaled[t] * (fixed[t] + field)
        held_two[x, y, z] = value
        ones.append(value)
    two_copies = halo(held_two, send_two, recv_two)
    for copy in two_copies:
        copy.start()
    pairs = [(x, y, z) for x in range(wraps[0]) for y in range(wraps[1]) for z in range(0, wraps[2], 2)]
    sums = [None] * count
    for near_by in ((0,), (1,), (2,), (3,)):
        for move, copy in zip(moves, two_copies):
            if sum(part[0] != 0 for part in move) in near_by:
                copy.wait()
        for x, y, z in pairs:
            if distance((x, y, z)) in near_by:
                set_features(
                    flat_of((x, y, z)) // 2,
                    jnp.concatenate([held_two[x, y, z], held_two[x, y, z + 1]], axis=1),
                )
        for t in range(count):
            found = partial_sums(t, near_by)
            sums[t] = found if sums[t] is None else [a + b for a, b in zip(sums[t], found)]
    field = [field_of(t, sums[t]) for t in range(count)]
    changed = jnp.zeros((ROWS, slots), jnp.float32)
    size = jnp.zeros((ROWS, slots), jnp.float32)
    for t, (x, y, z) in enumerate(places):
        before = ones[t]
        after = (1.0 - RELAXATION) * before + scaled[t] * (fixed[t] + field[t])
        for c in range(rows):
            out_ref[c, x, y, z, :] = after[row_of(c)]
        changed = changed + (after - before) * (after - before)
        size = size + after * after

    def all_of(value):
        return jnp.sum(jnp.sum(value, axis=0, keepdims=True), axis=1, keepdims=True)

    pair = jnp.where(lane == 0, all_of(changed), jnp.where(lane == 1, all_of(size), 0.0))
    share(1, 0, slots_c, pair)
    share(1, 1, slots_d, collect(1, 0, slots_c))
    pair = collect(1, 1, slots_d)
    above = jnp.sum(jnp.where(lane == 0, pair, 0.0), axis=1, keepdims=True)
    below = jnp.sum(jnp.where(lane == 1, pair, 0.0), axis=1, keepdims=True)
    change_ref[...] = jnp.broadcast_to(jnp.sqrt(above / (below + 1.0)), (1, slots))


def solution(mesh):
    devices = tuple(mesh.shape[axis] for axis in AXES)

    def on_device(fractions, polarizability, occupancy, pair_mask, perm_field, history):
        tiles = fractions.shape[1:4]
        slots = fractions.shape[4]
        count = tiles[0] * tiles[1] * tiles[2]
        wraps = tuple(n + 2 for n in tiles)
        total_tiles = wraps[0] * wraps[1] * wraps[2]
        moves = len(halo_moves(tiles))
        past = history.shape[0] - 1
        vmem = pl.BlockSpec(memory_space=pltpu.VMEM)
        f32 = jnp.float32
        groups = [devices[0], devices[1] * devices[2]]
        induced, change = pl.pallas_call(
            functools.partial(kernel, devices),
            out_shape=(
                jax.ShapeDtypeStruct(perm_field.shape, f32),
                jax.ShapeDtypeStruct((1, slots), f32),
            ),
            in_specs=[pl.BlockSpec(memory_space=pltpu.HBM)] * 6,
            out_specs=(vmem, vmem),
            scratch_shapes=[
                pltpu.VMEM(fractions.shape, f32),
                pltpu.VMEM(polarizability.shape, f32),
                pltpu.VMEM(occupancy.shape, jnp.int32),
                pltpu.SMEM(pair_mask.shape, jnp.int32),
                pltpu.VMEM(perm_field.shape, f32),
                pltpu.VMEM(history.shape, f32),
                pltpu.VMEM(wraps + (ROWS, slots), f32),
                pltpu.VMEM(wraps + (past * ROWS, slots), f32),
                pltpu.VMEM(wraps + (ROWS, slots), f32),
                pltpu.VMEM((history.shape[0], count, ROWS, slots), f32),
                pltpu.VMEM((total_tiles, ROWS, slots), f32),
                pltpu.VMEM((total_tiles, 4, slots, slots), f32),
                pltpu.VMEM((total_tiles // 2, 16 * ROWS, 2 * slots), jnp.bfloat16),
                pltpu.VMEM((count, 27, 2 * slots, 2 * slots), jnp.bfloat16),
            ]
            + [pltpu.VMEM((n, 1, slots), f32) for n in groups * 2]
            + [
                pltpu.SemaphoreType.DMA((6,)),
                pltpu.SemaphoreType.DMA((2, 2)),
                pltpu.SemaphoreType.DMA((2, 2)),
            ]
            + [pltpu.SemaphoreType.DMA((moves,))] * 6,
            compiler_params=pltpu.CompilerParams(
                collective_id=0, has_side_effects=True, vmem_limit_bytes=67043328
            ),
        )(fractions, polarizability, occupancy, pair_mask, perm_field, history)
        return induced, change[0, 0]

    in_specs = (
        P(None, "gx", "gy", "gz", None),
        P("gx", "gy", "gz", None),
        P("gx", "gy", "gz", None),
        P("gx", "gy", "gz", None),
        P(None, "gx", "gy", "gz", None),
        P(None, None, "gx", "gy", "gz", None),
    )
    out_specs = (P(None, "gx", "gy", "gz", None), P())
    return jax.shard_map(
        on_device, mesh=mesh, in_specs=in_specs, out_specs=out_specs, check_vma=False
    )
```

```python
import functools

import jax
import jax.numpy as jnp
from jax import lax
from jax.experimental import pallas as pl
from jax.experimental.pallas import tpu as pltpu
from jax.sharding import PartitionSpec as P

CELL_EDGE = 10.0
SOFTENING = 0.3
THOLE_DAMP = 0.39
RELAXATION = 0.7
LOG2E = 1.4426950408889634
MESH = pl.DeviceIdType.MESH
AXES = ("gx", "gy", "gz")
ROWS = 8
BLOCK = 32
GROUPS = ((0,), (1, 2))


def halo_moves(tiles):
    options = []
    for n in tiles:
        options.append([(0, 0, n, 0), (1, n - 1, 1, n + 1), (-1, 0, 1, n)])
    return [
        (a, b, c) for a in options[0] for b in options[1] for c in options[2] if (a[0], b[0], c[0]) != (0, 0, 0)
    ]


def solve_fit(total, past, lane, pair_lane):
    def pick(a, b):
        index = pair_lane[(min(a, b), max(a, b))]
        return jnp.sum(jnp.where(lane == index, total, 0.0), axis=1, keepdims=True)

    diagonal = [pick(a, a) for a in range(past)]
    trace = diagonal[0]
    for value in diagonal[1:]:
        trace = trace + value
    ridge = 0.001 * trace / past + 1.0
    lower, inverse = {}, []
    for j in range(past):
        pivot = diagonal[j] + ridge
        for m in range(j):
            pivot = pivot - lower[j, m] * lower[j, m]
        inverse.append(lax.rsqrt(pivot))
        for i in range(j + 1, past):
            value = pick(i, j)
            for m in range(j):
                value = value - lower[i, m] * lower[j, m]
            lower[i, j] = value * inverse[j]
    forward = []
    for i in range(past):
        value = pick(i, past)
        for m in range(i):
            value = value - lower[i, m] * forward[m]
        forward.append(value * inverse[i])
    coeffs = [None] * past
    for i in reversed(range(past)):
        value = forward[i]
        for m in range(i + 1, past):
            value = value - lower[m, i] * coeffs[m]
        coeffs[i] = value * inverse[i]
    return coeffs


def kernel(
    devices,
    frac_in, pol_in, occ_in, mask_in, perm_in, hist_in,
    out_ref, change_ref,
    frac_ref, pol_ref, occ_ref, mask_ref, perm_ref, hist_ref,
    geom, held_past, held_two, past_sets, spots, columns, features, weights,
    slots_a, slots_b, slots_c, slots_d, measure,
    load_sem, send_all, recv_all, send_near, recv_near,
):
    tiles = tuple(frac_ref.shape[1:4])
    wraps = tuple(n + 2 for n in tiles)
    slots = frac_ref.shape[4]
    steps = hist_ref.shape[0]
    rows = hist_ref.shape[1]
    past = steps - 1
    at = [lax.axis_index(axis) for axis in AXES]
    moves = halo_moves(tiles)
    lane = lax.broadcasted_iota(jnp.int32, (1, slots), 1)

    def size_of(axes):
        total = 1
        for axis in axes:
            total *= devices[axis]
        return total

    def shifted(shift):
        places = []
        for axis in range(3):
            place = at[axis] + shift[axis]
            places.append(jnp.where(place >= devices[axis], place - devices[axis], place))
        return tuple(places)

    def hops(shift):
        return sum(min(part, n - part) for part, n in zip(shift, devices))

    def shifts_of(axes):
        spans = [range(devices[axis]) if axis in axes else range(1) for axis in range(3)]
        every = [(x, y, z) for x in spans[0] for y in spans[1] for z in spans[2] if (x, y, z) != (0, 0, 0)]
        return sorted(every, key=lambda shift: -hops(shift))

    def rank_in(axes):
        rank = 0
        for axis in axes:
            rank = rank * devices[axis] + at[axis]
        return rank

    near = [tuple((move[axis][0] + devices[axis]) % devices[axis] for axis in range(3)) for move in moves]
    greeted = list(dict.fromkeys([shift for axes in GROUPS for shift in shifts_of(axes)] + near))

    barrier = pltpu.get_barrier_semaphore()
    loads = [
        pltpu.make_async_copy(source, target, load_sem.at[number])
        for number, (source, target) in enumerate(
            (
                (hist_in, hist_ref), (occ_in, occ_ref), (frac_in, frac_ref),
                (pol_in, pol_ref), (perm_in, perm_ref), (mask_in, mask_ref),
            )
        )
    ]
    for load in loads:
        load.start()

    for shift in greeted:
        pl.semaphore_signal(barrier, inc=1, device_id=shifted(shift), device_id_type=MESH)
    for load in loads:
        load.wait()

    def share(index, stage, held, value):
        axes = GROUPS[stage]
        rank = rank_in(axes)
        held[pl.ds(rank, 1)] = value.reshape(1, 1, slots)
        for shift in shifts_of(axes):
            pltpu.make_async_remote_copy(
                src_ref=held.at[pl.ds(rank, 1)],
                dst_ref=held.at[pl.ds(rank, 1)],
                send_sem=send_all.at[index, stage],
                recv_sem=recv_all.at[index, stage],
                device_id=shifted(shift),
                device_id_type=MESH,
            ).start()

    def collect(index, stage, held):
        others = size_of(GROUPS[stage]) - 1
        whole = pltpu.make_async_remote_copy(
            src_ref=held.at[pl.ds(0, others)],
            dst_ref=held.at[pl.ds(0, others)],
            send_sem=send_all.at[index, stage],
            recv_sem=recv_all.at[index, stage],
            device_id=shifted((0, 0, 1)),
            device_id_type=MESH,
        )
        whole.wait_send()
        whole.wait_recv()
        return jnp.sum(held[...], axis=0)

    def halo(held, send, recv, crossed):
        for move, shift in zip(moves, near):
            if sum(part[0] != 0 for part in move) not in crossed:
                continue
            source = tuple(pl.ds(part[1], part[2]) for part in move)
            place = tuple(pl.ds(part[3], part[2]) for part in move)
            pltpu.make_async_remote_copy(
                src_ref=held.at[source],
                dst_ref=held.at[place],
                send_sem=send,
                recv_sem=recv,
                device_id=shifted(shift),
                device_id_type=MESH,
            ).start()

    def halo_wait(held, send, recv, crossed):
        amount = 0
        for move in moves:
            if sum(part[0] != 0 for part in move) in crossed:
                amount += move[0][2] * move[1][2] * move[2][2] * (held.shape[3] // ROWS)
        whole = pltpu.make_async_remote_copy(
            src_ref=measure.at[pl.ds(0, amount)],
            dst_ref=measure.at[pl.ds(0, amount)],
            send_sem=send,
            recv_sem=recv,
            device_id=shifted(near[0]),
            device_id_type=MESH,
        )
        whole.wait_send()
        whole.wait_recv()

    def row_of(c):
        return 2 * (c % 3) + c // 3

    order = sorted(range(rows), key=row_of)
    places = [(x, y, z) for x in range(tiles[0]) for y in range(tiles[1]) for z in range(tiles[2])]
    count = len(places)
    zero_row = jnp.zeros((1, slots), jnp.float32)
    spare = jnp.zeros((ROWS - rows, slots), jnp.float32)
    scaled = []
    for t, (x, y, z) in enumerate(places):
        full = occ_ref[x, y, z, :].reshape(1, slots).astype(jnp.float32)
        pol = pol_ref[x, y, z, :].reshape(1, slots)
        scaled.append(RELAXATION * full * pol)
        parts = []
        for c in range(3):
            parts += [frac_ref[c, x, y, z, :].reshape(1, slots) * CELL_EDGE] * 2
        geom[x, y, z] = jnp.concatenate(parts + [lax.rsqrt(pol), zero_row], axis=0)
        for h in range(steps):
            moment = jnp.concatenate(
                [hist_ref[h, c, x, y, z, :].reshape(1, slots) for c in order] + [spare], axis=0
            ) * full
            past_sets[h, t] = moment
            if h > 0:
                held_past[x, y, z, pl.ds(ROWS * (h - 1), ROWS), :] = moment
    pair_lane = {}
    gram = zero_row
    for a in range(steps):
        for b in range(a, steps):
            product = past_sets[a, 0] * past_sets[b, 0]
            for t in range(1, count):
                product = product + past_sets[a, t] * past_sets[b, t]
            value = jnp.sum(jnp.sum(product, axis=0, keepdims=True), axis=1, keepdims=True)
            pair_lane[(a, b)] = len(pair_lane)
            gram = jnp.where(lane == pair_lane[(a, b)], value, gram)

    row = lax.broadcasted_iota(jnp.int32, (ROWS, slots), 0)
    wide_row = lax.broadcasted_iota(jnp.int32, (ROWS, 2 * slots), 0)

    square_row = lax.broadcasted_iota(jnp.int32, (slots, slots), 0)
    square_lane = lax.broadcasted_iota(jnp.int32, (slots, slots), 1)

    def flat_of(place):
        return (place[0] * wraps[1] + place[1]) * wraps[2] + place[2]

    def wrap(value, size):
        return jnp.where(value < 0, value + size, value)

    def rounded(value):
        return value.astype(jnp.bfloat16).astype(jnp.float32)

    piece_row = lax.broadcasted_iota(jnp.int32, (4 * ROWS, 4 * slots), 0)
    piece_lane = lax.broadcasted_iota(jnp.int32, (4 * ROWS, 4 * slots), 1)
    chosen_rows = jnp.where(
        jnp.logical_and(
            lax.bitwise_and(piece_row, ROWS - 1) == 2 * lax.shift_right_logical(piece_lane, 7), piece_row < 3 * ROWS
        ),
        1.0,
        0.0,
    ).astype(jnp.bfloat16)

    def prepare(place):
        flat = flat_of(place)
        tile = geom[place[0], place[1], place[2]]
        moved = []
        for axis in range(3):
            number = jnp.where(place[axis] == wraps[axis] - 1, -1, place[axis])
            moved.append(CELL_EDGE * (number.astype(jnp.float32) - 0.5 * tiles[axis]))
        offset = jnp.where(row < 2, moved[0], jnp.where(row < 4, moved[1], jnp.where(row < 6, moved[2], 0.0)))
        tile = tile + offset
        spots[flat] = tile
        middle = tile - rounded(tile)
        last = middle - rounded(middle)
        upright = jnp.concatenate([tile, middle, last, jnp.zeros_like(tile)], axis=0).T
        spread = jnp.dot(upright.astype(jnp.bfloat16), chosen_rows, preferred_element_type=jnp.float32)
        for c in range(4):
            columns[flat, c] = spread[:, c * slots : (c + 1) * slots]

    def split(t):
        return lax.shift_right_logical(t, 1), lax.bitwise_and(t, 1)

    def pair_weights(t, along, itself):
        first_y, first_z = split(t)
        base = (jnp.int32(0), first_y, first_z)
        place = tuple(wrap(base[i] + along[i], wraps[i]) for i in range(3))
        k = 9 * (along[0] + 1) + 3 * (along[1] + 1) + along[2] + 1
        source = flat_of(place)
        own = flat_of(base)
        here = [spots[own, pl.ds(2 * c, 1), :] for c in range(4)]
        allowed = mask_ref[0, first_y, first_z, k].astype(jnp.float32)
        damp = here[3] * (-THOLE_DAMP * allowed)
        for first in range(0, slots, BLOCK):
            part = pl.ds(first, BLOCK)
            dx = columns[source, 0, part, :] - here[0]
            dy = columns[source, 1, part, :] - here[1]
            dz = columns[source, 2, part, :] - here[2]
            square = dx * dx + dy * dy + (dz * dz + SOFTENING)
            root = lax.rsqrt(square)
            root_two = root * root
            cube = root_two * root
            arg = (square * square) * root * (damp * columns[source, 3, part, :])
            fade = jnp.exp2(arg * LOG2E)
            three = 1.0 - fade
            five = three + arg * fade
            radial, direct = five * cube * root_two, three * cube
            if itself:
                apart = square_row[first : first + BLOCK] != square_lane[first : first + BLOCK]
                radial, direct = jnp.where(apart, radial, 0.0), jnp.where(apart, direct, 0.0)
            both = jnp.concatenate([radial, direct], axis=1)
            high = both.astype(jnp.bfloat16)
            weights[t, k, part, :] = high
            weights[t, k, pl.ds(slots + first, BLOCK), :] = (both - high.astype(jnp.float32)).astype(jnp.bfloat16)

    def outward(t):
        first_y, first_z = split(t)
        return 2 * first_y - 1, 2 * first_z - 1

    def inner_pairs(t, carry):
        out_y, out_z = outward(t)
        for q in range(4):
            pair_weights(t, (0, -out_y * (q // 2), -out_z * (q % 2)), q == 0)
        return carry

    def edge_pairs(t, carry):
        out_y, out_z = outward(t)
        for along in ((out_y, -1), (out_y, 0), (out_y, 1), (0, out_z), (-out_y, out_z)):
            pair_weights(t, (0,) + along, False)
        return carry

    def plane_pairs(along_x):
        def one(t, carry):
            for q in range(9):
                pair_weights(t, (along_x, q // 3 - 1, q % 3 - 1), False)
            return carry

        return one

    for place in places:
        prepare(tuple(jnp.int32(part) for part in place))
    lax.fori_loop(0, count, inner_pairs, 0)

    pl.semaphore_wait(barrier, len(greeted))
    share(0, 0, slots_a, gram)
    everywhere = (1, 2, 3)
    halo(geom, send_near.at[0], recv_near.at[0], everywhere)
    halo(held_past, send_near.at[1], recv_near.at[1], everywhere)
    halo_wait(geom, send_near.at[0], recv_near.at[0], everywhere)

    for y in range(wraps[1]):
        for z in range(wraps[2]):
            if y >= tiles[1] or z >= tiles[2]:
                prepare((jnp.int32(0), jnp.int32(y), jnp.int32(z)))

    def prepare_eight(step, carry):
        half_x, half_y = split(step)
        for q in range(8):
            prepare((1 + half_x, 2 * half_y + q // 4, jnp.int32(q % 4)))
        return carry

    lax.fori_loop(0, 4, prepare_eight, 0)
    share(0, 1, slots_b, collect(0, 0, slots_a))
    lax.fori_loop(0, count, edge_pairs, 0)
    lax.fori_loop(0, count, plane_pairs(-1), 0)
    lax.fori_loop(0, count, plane_pairs(1), 0)

    def cycle(value):
        value = value + pltpu.roll(value, 4, 0)
        return value + pltpu.roll(value, 2, 0)

    def set_features(pair, moment):
        twice = [2 * pair, 2 * pair + 1]
        spot = jnp.concatenate([spots[flat] for flat in twice], axis=1)
        spot = jnp.where(wide_row < rows, spot, 0.0)
        by = [
            jnp.concatenate([spots[flat, pl.ds(2 * c, 1), :] for flat in twice], axis=1) * moment
            for c in range(3)
        ]
        first = jnp.concatenate([moment, by[0]], axis=0)
        second = jnp.concatenate(by[1:], axis=0)
        third = cycle(spot * moment) * spot
        middle = third - rounded(third)
        last = middle - rounded(middle)
        blocks = []
        for piece in range(3):
            blocks += [first, second]
            if piece < 2:
                first = first - rounded(first)
                second = second - rounded(second)
        blocks.append(jnp.concatenate([third, middle], axis=0))
        blocks.append(jnp.concatenate([last, jnp.zeros_like(last)], axis=0))
        for number, value in enumerate(blocks):
            features[pair, pl.ds(2 * ROWS * number, 2 * ROWS), :] = value.astype(jnp.bfloat16)

    def along_of(k):
        return (k // 9 - 1, k // 3 % 3 - 1, k % 3 - 1)

    def target_of(place, k):
        along = along_of(k)
        return tuple((place[i] + along[i] + wraps[i]) % wraps[i] for i in range(3))

    def distance(place):
        return sum(part >= n for part, n in zip(place, tiles))

    def partial_sums(t, chosen):
        acc = None
        for k in range(27):
            place = target_of(places[t], k)
            if distance(place) in chosen:
                flat = flat_of(place)
                side = features[flat // 2, :, pl.ds(flat % 2 * slots, slots)]
                part = jnp.dot(
                    jnp.concatenate([side, side], axis=1), weights[t, k], preferred_element_type=jnp.float32
                )
                acc = part if acc is None else acc + part
        group = [acc[ROWS * g : ROWS * (g + 1)] for g in range(2 * ROWS)]
        sums = [(group[8 + g] + group[4 + g] + group[g])[:, 0:slots] for g in range(4)]
        sums.append((group[14] + group[13] + group[12])[:, 0:slots])
        sums.append((group[8] + group[4] + group[0])[:, slots : 2 * slots])
        return sums

    def field_of(t, sums):
        plain, by_x, by_y, by_z, whole, direct = sums
        spot = jnp.where(row < rows, spots[flat_of(places[t])], 0.0)
        mine = [cycle(spot * value) for value in (by_x, by_y, by_z)]
        middle = jnp.where(row < 2, by_x, jnp.where(row < 4, by_y, by_z))
        drawn = jnp.where(row < 2, mine[0], jnp.where(row < 4, mine[1], mine[2]))
        radial = whole - drawn + spot * cycle(spot * plain - middle)
        return jnp.where(row < rows, 3.0 * radial - direct, 0.0)

    fixed = [
        jnp.concatenate([perm_ref[c, x, y, z, :].reshape(1, slots) for c in order] + [spare], axis=0)
        for (x, y, z) in places
    ]
    halo_wait(held_past, send_near.at[1], recv_near.at[1], everywhere)
    total = collect(0, 1, slots_b)
    coeffs = [jnp.broadcast_to(value, (ROWS, slots)) for value in solve_fit(total, past, lane, pair_lane)]

    def predicted(x, y, z):
        value = coeffs[0] * held_past[x, y, z, pl.ds(0, ROWS), :]
        for h in range(1, past):
            value = value + coeffs[h] * held_past[x, y, z, pl.ds(ROWS * h, ROWS), :]
        return value

    def predict(step, carry):
        x, y = lax.shift_right_logical(step, 2), lax.bitwise_and(step, 3)
        for half in range(2):
            moment = jnp.concatenate([predicted(x, y, 2 * half), predicted(x, y, 2 * half + 1)], axis=1)
            set_features(2 * step + half, moment)
        return carry

    lax.fori_loop(0, wraps[0] * wraps[1], predict, 0)
    ones = []
    for t, (x, y, z) in enumerate(places):
        field = field_of(t, partial_sums(t, (0, 1, 2, 3)))
        value = (1.0 - RELAXATION) * predicted(x, y, z) + scaled[t] * (fixed[t] + field)
        held_two[x, y, z] = value
        ones.append(value)
    for crossed in (3, 2, 1):
        halo(held_two, send_near.at[1 + crossed], recv_near.at[1 + crossed], (crossed,))
    pairs = [(x, y, z) for x in range(wraps[0]) for y in range(wraps[1]) for z in range(0, wraps[2], 2)]
    sums = [None] * count
    for near_by in ((0,), (1,), (2,), (3,)):
        if near_by != (0,):
            halo_wait(held_two, send_near.at[1 + near_by[0]], recv_near.at[1 + near_by[0]], near_by)
        for x, y, z in pairs:
            if distance((x, y, z)) in near_by:
                set_features(
                    flat_of((x, y, z)) // 2,
                    jnp.concatenate([held_two[x, y, z], held_two[x, y, z + 1]], axis=1),
                )
        for t in range(count):
            found = partial_sums(t, near_by)
            sums[t] = found if sums[t] is None else [a + b for a, b in zip(sums[t], found)]
    field = [field_of(t, sums[t]) for t in range(count)]
    changed = jnp.zeros((ROWS, slots), jnp.float32)
    size = jnp.zeros((ROWS, slots), jnp.float32)
    for t, (x, y, z) in enumerate(places):
        before = ones[t]
        after = (1.0 - RELAXATION) * before + scaled[t] * (fixed[t] + field[t])
        for c in range(rows):
            out_ref[c, x, y, z, :] = after[row_of(c)]
        changed = changed + (after - before) * (after - before)
        size = size + after * after

    def all_of(value):
        return jnp.sum(jnp.sum(value, axis=0, keepdims=True), axis=1, keepdims=True)

    pair = jnp.where(lane == 0, all_of(changed), jnp.where(lane == 1, all_of(size), 0.0))
    share(1, 0, slots_c, pair)
    share(1, 1, slots_d, collect(1, 0, slots_c))
    pair = collect(1, 1, slots_d)
    above = jnp.sum(jnp.where(lane == 0, pair, 0.0), axis=1, keepdims=True)
    below = jnp.sum(jnp.where(lane == 1, pair, 0.0), axis=1, keepdims=True)
    change_ref[...] = jnp.broadcast_to(jnp.sqrt(above / (below + 1.0)), (1, slots))


def solution(mesh):
    devices = tuple(mesh.shape[axis] for axis in AXES)

    def on_device(fractions, polarizability, occupancy, pair_mask, perm_field, history):
        tiles = fractions.shape[1:4]
        slots = fractions.shape[4]
        count = tiles[0] * tiles[1] * tiles[2]
        wraps = tuple(n + 2 for n in tiles)
        total_tiles = wraps[0] * wraps[1] * wraps[2]
        past = history.shape[0] - 1
        vmem = pl.BlockSpec(memory_space=pltpu.VMEM)
        f32 = jnp.float32
        groups = [devices[0], devices[1] * devices[2]]
        induced, change = pl.pallas_call(
            functools.partial(kernel, devices),
            out_shape=(
                jax.ShapeDtypeStruct(perm_field.shape, f32),
                jax.ShapeDtypeStruct((1, slots), f32),
            ),
            in_specs=[pl.BlockSpec(memory_space=pltpu.HBM)] * 6,
            out_specs=(vmem, vmem),
            scratch_shapes=[
                pltpu.VMEM(fractions.shape, f32),
                pltpu.VMEM(polarizability.shape, f32),
                pltpu.VMEM(occupancy.shape, jnp.int32),
                pltpu.SMEM(pair_mask.shape, jnp.int32),
                pltpu.VMEM(perm_field.shape, f32),
                pltpu.VMEM(history.shape, f32),
                pltpu.VMEM(wraps + (ROWS, slots), f32),
                pltpu.VMEM(wraps + (past * ROWS, slots), f32),
                pltpu.VMEM(wraps + (ROWS, slots), f32),
                pltpu.VMEM((history.shape[0], count, ROWS, slots), f32),
                pltpu.VMEM((total_tiles, ROWS, slots), f32),
                pltpu.VMEM((total_tiles, 4, slots, slots), f32),
                pltpu.VMEM((total_tiles // 2, 16 * ROWS, 2 * slots), jnp.bfloat16),
                pltpu.VMEM((count, 27, 2 * slots, 2 * slots), jnp.bfloat16),
            ]
            + [pltpu.VMEM((n, 1, slots), f32) for n in groups * 2]
            + [pltpu.VMEM(((total_tiles - count) * past, ROWS, slots), f32)]
            + [
                pltpu.SemaphoreType.DMA((6,)),
                pltpu.SemaphoreType.DMA((2, 2)),
                pltpu.SemaphoreType.DMA((2, 2)),
            ]
            + [pltpu.SemaphoreType.DMA((5,))] * 2,
            compiler_params=pltpu.CompilerParams(
                collective_id=0, has_side_effects=True, vmem_limit_bytes=67043328
            ),
        )(fractions, polarizability, occupancy, pair_mask, perm_field, history)
        return induced, change[0, 0]

    in_specs = (
        P(None, "gx", "gy", "gz", None),
        P("gx", "gy", "gz", None),
        P("gx", "gy", "gz", None),
        P("gx", "gy", "gz", None),
        P(None, "gx", "gy", "gz", None),
        P(None, None, "gx", "gy", "gz", None),
    )
    out_specs = (P(None, "gx", "gy", "gz", None), P())
    return jax.shard_map(
        on_device, mesh=mesh, in_specs=in_specs, out_specs=out_specs, check_vma=False
    )
```

```python
import functools

import jax
import jax.numpy as jnp
from jax import lax
from jax.experimental import pallas as pl
from jax.experimental.pallas import tpu as pltpu
from jax.sharding import PartitionSpec as P

CELL_EDGE = 10.0
SOFTENING = 0.3
THOLE_DAMP = 0.39
RELAXATION = 0.7
LOG2E = 1.4426950408889634
MESH = pl.DeviceIdType.MESH
AXES = ("gx", "gy", "gz")
ROWS = 8
BLOCK = 32
GROUPS = ((0,), (1, 2))


def halo_moves(tiles):
    options = []
    for n in tiles:
        options.append([(0, 0, n, 0), (1, n - 1, 1, n + 1), (-1, 0, 1, n)])
    return [
        (a, b, c) for a in options[0] for b in options[1] for c in options[2] if (a[0], b[0], c[0]) != (0, 0, 0)
    ]


def solve_fit(total, past, lane, pair_lane):
    def pick(a, b):
        index = pair_lane[(min(a, b), max(a, b))]
        return jnp.sum(jnp.where(lane == index, total, 0.0), axis=1, keepdims=True)

    diagonal = [pick(a, a) for a in range(past)]
    trace = diagonal[0]
    for value in diagonal[1:]:
        trace = trace + value
    ridge = 0.001 * trace / past + 1.0
    lower, inverse = {}, []
    for j in range(past):
        pivot = diagonal[j] + ridge
        for m in range(j):
            pivot = pivot - lower[j, m] * lower[j, m]
        inverse.append(lax.rsqrt(pivot))
        for i in range(j + 1, past):
            value = pick(i, j)
            for m in range(j):
                value = value - lower[i, m] * lower[j, m]
            lower[i, j] = value * inverse[j]
    forward = []
    for i in range(past):
        value = pick(i, past)
        for m in range(i):
            value = value - lower[i, m] * forward[m]
        forward.append(value * inverse[i])
    coeffs = [None] * past
    for i in reversed(range(past)):
        value = forward[i]
        for m in range(i + 1, past):
            value = value - lower[m, i] * coeffs[m]
        coeffs[i] = value * inverse[i]
    return coeffs


def kernel(
    devices,
    frac_in, pol_in, occ_in, mask_in, perm_in, hist_in,
    out_ref, change_ref,
    frac_ref, pol_ref, occ_ref, mask_ref, perm_ref, hist_ref,
    geom, held_past, held_two, past_sets, spots, columns, features, weights,
    slots_a, slots_b, slots_c, slots_d, measure,
    load_sem, send_all, recv_all, send_near, recv_near,
):
    tiles = tuple(frac_ref.shape[1:4])
    wraps = tuple(n + 2 for n in tiles)
    slots = frac_ref.shape[4]
    steps = hist_ref.shape[0]
    rows = hist_ref.shape[1]
    past = steps - 1
    at = [lax.axis_index(axis) for axis in AXES]
    moves = halo_moves(tiles)
    lane = lax.broadcasted_iota(jnp.int32, (1, slots), 1)

    loads = [
        pltpu.make_async_copy(source, target, load_sem.at[number])
        for number, (source, target) in enumerate(
            (
                (hist_in, hist_ref), (occ_in, occ_ref), (frac_in, frac_ref),
                (pol_in, pol_ref), (perm_in, perm_ref), (mask_in, mask_ref),
            )
        )
    ]
    for load in loads:
        load.start()

    def size_of(axes):
        total = 1
        for axis in axes:
            total *= devices[axis]
        return total

    def shifted(shift):
        places = []
        for axis in range(3):
            place = at[axis] + shift[axis]
            places.append(jnp.where(place >= devices[axis], place - devices[axis], place))
        return tuple(places)

    def hops(shift):
        return sum(min(part, n - part) for part, n in zip(shift, devices))

    def shifts_of(axes):
        spans = [range(devices[axis]) if axis in axes else range(1) for axis in range(3)]
        every = [(x, y, z) for x in spans[0] for y in spans[1] for z in spans[2] if (x, y, z) != (0, 0, 0)]
        return sorted(every, key=lambda shift: -hops(shift))

    def rank_in(axes):
        rank = 0
        for axis in axes:
            rank = rank * devices[axis] + at[axis]
        return rank

    near = [tuple((move[axis][0] + devices[axis]) % devices[axis] for axis in range(3)) for move in moves]
    greeted = list(dict.fromkeys([shift for axes in GROUPS for shift in shifts_of(axes)] + near))

    barrier = pltpu.get_barrier_semaphore()
    for shift in greeted:
        pl.semaphore_signal(barrier, inc=1, device_id=shifted(shift), device_id_type=MESH)
    for load in loads:
        load.wait()

    def share(index, stage, held, value):
        axes = GROUPS[stage]
        rank = rank_in(axes)
        held[pl.ds(rank, 1)] = value.reshape(1, 1, slots)
        for shift in shifts_of(axes):
            pltpu.make_async_remote_copy(
                src_ref=held.at[pl.ds(rank, 1)],
                dst_ref=held.at[pl.ds(rank, 1)],
                send_sem=send_all.at[index, stage],
                recv_sem=recv_all.at[index, stage],
                device_id=shifted(shift),
                device_id_type=MESH,
            ).start()

    def collect(index, stage, held):
        others = size_of(GROUPS[stage]) - 1
        whole = pltpu.make_async_remote_copy(
            src_ref=held.at[pl.ds(0, others)],
            dst_ref=held.at[pl.ds(0, others)],
            send_sem=send_all.at[index, stage],
            recv_sem=recv_all.at[index, stage],
            device_id=shifted((0, 0, 1)),
            device_id_type=MESH,
        )
        whole.wait_send()
        whole.wait_recv()
        return jnp.sum(held[...], axis=0)

    def halo(held, send, recv, crossed):
        for move, shift in zip(moves, near):
            if sum(part[0] != 0 for part in move) not in crossed:
                continue
            source = tuple(pl.ds(part[1], part[2]) for part in move)
            place = tuple(pl.ds(part[3], part[2]) for part in move)
            pltpu.make_async_remote_copy(
                src_ref=held.at[source],
                dst_ref=held.at[place],
                send_sem=send,
                recv_sem=recv,
                device_id=shifted(shift),
                device_id_type=MESH,
            ).start()

    def halo_wait(held, send, recv, crossed):
        amount = 0
        for move in moves:
            if sum(part[0] != 0 for part in move) in crossed:
                amount += move[0][2] * move[1][2] * move[2][2] * (held.shape[3] // ROWS)
        whole = pltpu.make_async_remote_copy(
            src_ref=measure.at[pl.ds(0, amount)],
            dst_ref=measure.at[pl.ds(0, amount)],
            send_sem=send,
            recv_sem=recv,
            device_id=shifted(near[0]),
            device_id_type=MESH,
        )
        whole.wait_send()
        whole.wait_recv()

    def row_of(c):
        return 2 * (c % 3) + c // 3

    order = sorted(range(rows), key=row_of)
    places = [(x, y, z) for x in range(tiles[0]) for y in range(tiles[1]) for z in range(tiles[2])]
    count = len(places)
    zero_row = jnp.zeros((1, slots), jnp.float32)
    spare = jnp.zeros((ROWS - rows, slots), jnp.float32)
    scaled = []
    for t, (x, y, z) in enumerate(places):
        full = occ_ref[x, y, z, :].reshape(1, slots).astype(jnp.float32)
        pol = pol_ref[x, y, z, :].reshape(1, slots)
        scaled.append(RELAXATION * full * pol)
        parts = []
        for c in range(3):
            parts += [frac_ref[c, x, y, z, :].reshape(1, slots) * CELL_EDGE] * 2
        geom[x, y, z] = jnp.concatenate(parts + [lax.rsqrt(pol), zero_row], axis=0)
        for h in range(steps):
            moment = jnp.concatenate(
                [hist_ref[h, c, x, y, z, :].reshape(1, slots) for c in order] + [spare], axis=0
            ) * full
            past_sets[h, t] = moment
            if h > 0:
                held_past[x, y, z, pl.ds(ROWS * (h - 1), ROWS), :] = moment
    pair_lane = {}
    gram = zero_row
    for a in range(steps):
        for b in range(a, steps):
            product = past_sets[a, 0] * past_sets[b, 0]
            for t in range(1, count):
                product = product + past_sets[a, t] * past_sets[b, t]
            value = jnp.sum(jnp.sum(product, axis=0, keepdims=True), axis=1, keepdims=True)
            pair_lane[(a, b)] = len(pair_lane)
            gram = jnp.where(lane == pair_lane[(a, b)], value, gram)

    row = lax.broadcasted_iota(jnp.int32, (ROWS, slots), 0)
    wide_row = lax.broadcasted_iota(jnp.int32, (ROWS, 2 * slots), 0)

    square_row = lax.broadcasted_iota(jnp.int32, (slots, slots), 0)
    square_lane = lax.broadcasted_iota(jnp.int32, (slots, slots), 1)

    def flat_of(place):
        return (place[0] * wraps[1] + place[1]) * wraps[2] + place[2]

    def wrap(value, size):
        return jnp.where(value < 0, value + size, value)

    def rounded(value):
        return value.astype(jnp.bfloat16).astype(jnp.float32)

    piece_row = lax.broadcasted_iota(jnp.int32, (4 * ROWS, 4 * slots), 0)
    piece_lane = lax.broadcasted_iota(jnp.int32, (4 * ROWS, 4 * slots), 1)
    chosen_rows = jnp.where(
        jnp.logical_and(
            lax.bitwise_and(piece_row, ROWS - 1) == 2 * lax.shift_right_logical(piece_lane, 7), piece_row < 3 * ROWS
        ),
        1.0,
        0.0,
    ).astype(jnp.bfloat16)

    def prepare(place):
        flat = flat_of(place)
        tile = geom[place[0], place[1], place[2]]
        moved = []
        for axis in range(3):
            number = jnp.where(place[axis] == wraps[axis] - 1, -1, place[axis])
            moved.append(CELL_EDGE * (number.astype(jnp.float32) - 0.5 * tiles[axis]))
        offset = jnp.where(row < 2, moved[0], jnp.where(row < 4, moved[1], jnp.where(row < 6, moved[2], 0.0)))
        tile = tile + offset
        spots[flat] = tile
        middle = tile - rounded(tile)
        last = middle - rounded(middle)
        upright = jnp.concatenate([tile, middle, last, jnp.zeros_like(tile)], axis=0).T
        spread = jnp.dot(upright.astype(jnp.bfloat16), chosen_rows, preferred_element_type=jnp.float32)
        for c in range(4):
            columns[flat, c] = spread[:, c * slots : (c + 1) * slots]

    def split(t):
        return lax.shift_right_logical(t, 1), lax.bitwise_and(t, 1)

    def pair_weights(t, along, itself):
        first_y, first_z = split(t)
        base = (jnp.int32(0), first_y, first_z)
        place = tuple(wrap(base[i] + along[i], wraps[i]) for i in range(3))
        k = 9 * (along[0] + 1) + 3 * (along[1] + 1) + along[2] + 1
        source = flat_of(place)
        own = flat_of(base)
        here = [spots[own, pl.ds(2 * c, 1), :] for c in range(4)]
        allowed = mask_ref[0, first_y, first_z, k].astype(jnp.float32)
        damp = here[3] * (-THOLE_DAMP * allowed)
        for first in range(0, slots, BLOCK):
            part = pl.ds(first, BLOCK)
            dx = columns[source, 0, part, :] - here[0]
            dy = columns[source, 1, part, :] - here[1]
            dz = columns[source, 2, part, :] - here[2]
            square = dx * dx + dy * dy + (dz * dz + SOFTENING)
            root = lax.rsqrt(square)
            root_two = root * root
            cube = root_two * root
            arg = (square * square) * root * (damp * columns[source, 3, part, :])
            fade = jnp.exp2(arg * LOG2E)
            three = 1.0 - fade
            five = three + arg * fade
            radial, direct = five * cube * root_two, three * cube
            if itself:
                apart = square_row[first : first + BLOCK] != square_lane[first : first + BLOCK]
                radial, direct = jnp.where(apart, radial, 0.0), jnp.where(apart, direct, 0.0)
            both = jnp.concatenate([radial, direct], axis=1)
            high = both.astype(jnp.bfloat16)
            weights[t, k, part, :] = high
            weights[t, k, pl.ds(slots + first, BLOCK), :] = (both - high.astype(jnp.float32)).astype(jnp.bfloat16)

    def outward(t):
        first_y, first_z = split(t)
        return 2 * first_y - 1, 2 * first_z - 1

    def weigh(choose):
        def one(t, carry):
            for along in choose(*outward(t)):
                pair_weights(t, along, all(isinstance(part, int) and part == 0 for part in along))
            return carry

        lax.fori_loop(0, count, one, 0)

    def distance(place):
        return sum(part >= n for part, n in zip(place, tiles))

    def prepare_at(crossed):
        for x in range(wraps[0]):
            for y in range(wraps[1]):
                for z in range(wraps[2]):
                    if distance((x, y, z)) == crossed:
                        prepare((jnp.int32(x), jnp.int32(y), jnp.int32(z)))

    prepare_at(0)
    pl.semaphore_wait(barrier, len(greeted))
    share(0, 0, slots_a, gram)
    for crossed in (1, 2, 3):
        halo(geom, send_near.at[crossed - 1], recv_near.at[crossed - 1], (crossed,))
    everywhere = (1, 2, 3)
    halo(held_past, send_near.at[3], recv_near.at[3], everywhere)
    weigh(lambda y, z: ((0, 0, 0), (0, 0, -z), (0, -y, 0), (0, -y, -z)))
    halo_wait(geom, send_near.at[0], recv_near.at[0], (1,))
    prepare_at(1)
    weigh(lambda y, z: tuple((-1, -y * b, -z * c) for b in (0, 1) for c in (0, 1)) + ((0, y, 0), (0, y, -z)))
    share(0, 1, slots_b, collect(0, 0, slots_a))
    weigh(lambda y, z: tuple((1, -y * b, -z * c) for b in (0, 1) for c in (0, 1)) + ((0, 0, z), (0, -y, z)))
    halo_wait(geom, send_near.at[1], recv_near.at[1], (2,))
    prepare_at(2)
    weigh(
        lambda y, z: tuple((x,) + side for x in (-1, 1) for side in ((y, 0), (y, -z), (0, z), (-y, z)))
        + ((0, y, z),)
    )
    halo_wait(geom, send_near.at[2], recv_near.at[2], (3,))
    prepare_at(3)
    weigh(lambda y, z: ((-1, y, z), (1, y, z)))

    def cycle(value):
        value = value + pltpu.roll(value, 4, 0)
        return value + pltpu.roll(value, 2, 0)

    def set_features(pair, moment):
        twice = [2 * pair, 2 * pair + 1]
        spot = jnp.concatenate([spots[flat] for flat in twice], axis=1)
        spot = jnp.where(wide_row < rows, spot, 0.0)
        by = [
            jnp.concatenate([spots[flat, pl.ds(2 * c, 1), :] for flat in twice], axis=1) * moment
            for c in range(3)
        ]
        first = jnp.concatenate([moment, by[0]], axis=0)
        second = jnp.concatenate(by[1:], axis=0)
        third = cycle(spot * moment) * spot
        middle = third - rounded(third)
        last = middle - rounded(middle)
        blocks = []
        for piece in range(3):
            blocks += [first, second]
            if piece < 2:
                first = first - rounded(first)
                second = second - rounded(second)
        blocks.append(jnp.concatenate([third, middle], axis=0))
        blocks.append(jnp.concatenate([last, jnp.zeros_like(last)], axis=0))
        for number, value in enumerate(blocks):
            features[pair, pl.ds(2 * ROWS * number, 2 * ROWS), :] = value.astype(jnp.bfloat16)

    def along_of(k):
        return (k // 9 - 1, k // 3 % 3 - 1, k % 3 - 1)

    def target_of(place, k):
        along = along_of(k)
        return tuple((place[i] + along[i] + wraps[i]) % wraps[i] for i in range(3))

    def partial_sums(t, chosen):
        acc = None
        for k in range(27):
            place = target_of(places[t], k)
            if distance(place) in chosen:
                flat = flat_of(place)
                side = features[flat // 2, :, pl.ds(flat % 2 * slots, slots)]
                part = jnp.dot(
                    jnp.concatenate([side, side], axis=1), weights[t, k], preferred_element_type=jnp.float32
                )
                acc = part if acc is None else acc + part
        group = [acc[ROWS * g : ROWS * (g + 1)] for g in range(2 * ROWS)]
        sums = [(group[8 + g] + group[4 + g] + group[g])[:, 0:slots] for g in range(4)]
        sums.append((group[14] + group[13] + group[12])[:, 0:slots])
        sums.append((group[8] + group[4] + group[0])[:, slots : 2 * slots])
        return sums

    def field_of(t, sums):
        plain, by_x, by_y, by_z, whole, direct = sums
        spot = jnp.where(row < rows, spots[flat_of(places[t])], 0.0)
        mine = [cycle(spot * value) for value in (by_x, by_y, by_z)]
        middle = jnp.where(row < 2, by_x, jnp.where(row < 4, by_y, by_z))
        drawn = jnp.where(row < 2, mine[0], jnp.where(row < 4, mine[1], mine[2]))
        radial = whole - drawn + spot * cycle(spot * plain - middle)
        return jnp.where(row < rows, 3.0 * radial - direct, 0.0)

    fixed = [
        jnp.concatenate([perm_ref[c, x, y, z, :].reshape(1, slots) for c in order] + [spare], axis=0)
        for (x, y, z) in places
    ]
    halo_wait(held_past, send_near.at[3], recv_near.at[3], everywhere)
    total = collect(0, 1, slots_b)
    coeffs = [jnp.broadcast_to(value, (ROWS, slots)) for value in solve_fit(total, past, lane, pair_lane)]

    def predicted(x, y, z):
        value = coeffs[0] * held_past[x, y, z, pl.ds(0, ROWS), :]
        for h in range(1, past):
            value = value + coeffs[h] * held_past[x, y, z, pl.ds(ROWS * h, ROWS), :]
        return value

    pairs = [(x, y, z) for x in range(wraps[0]) for y in range(wraps[1]) for z in range(0, wraps[2], 2)]
    for x, y, z in pairs:
        set_features(
            flat_of((x, y, z)) // 2, jnp.concatenate([predicted(x, y, z), predicted(x, y, z + 1)], axis=1)
        )
    ones = []
    for t, (x, y, z) in enumerate(places):
        field = field_of(t, partial_sums(t, (0, 1, 2, 3)))
        value = (1.0 - RELAXATION) * predicted(x, y, z) + scaled[t] * (fixed[t] + field)
        held_two[x, y, z] = value
        ones.append(value)
    for crossed in (3, 2, 1):
        halo(held_two, send_near.at[3 + crossed], recv_near.at[3 + crossed], (crossed,))
    sums = [None] * count
    for near_by in ((0,), (1,), (2,), (3,)):
        if near_by != (0,):
            halo_wait(held_two, send_near.at[3 + near_by[0]], recv_near.at[3 + near_by[0]], near_by)
        for x, y, z in pairs:
            if distance((x, y, z)) in near_by:
                set_features(
                    flat_of((x, y, z)) // 2,
                    jnp.concatenate([held_two[x, y, z], held_two[x, y, z + 1]], axis=1),
                )
        for t in range(count):
            found = partial_sums(t, near_by)
            sums[t] = found if sums[t] is None else [a + b for a, b in zip(sums[t], found)]
    field = [field_of(t, sums[t]) for t in range(count)]
    changed = jnp.zeros((ROWS, slots), jnp.float32)
    size = jnp.zeros((ROWS, slots), jnp.float32)
    for t, (x, y, z) in enumerate(places):
        before = ones[t]
        after = (1.0 - RELAXATION) * before + scaled[t] * (fixed[t] + field[t])
        for c in range(rows):
            out_ref[c, x, y, z, :] = after[row_of(c)]
        changed = changed + (after - before) * (after - before)
        size = size + after * after

    def all_of(value):
        return jnp.sum(jnp.sum(value, axis=0, keepdims=True), axis=1, keepdims=True)

    pair = jnp.where(lane == 0, all_of(changed), jnp.where(lane == 1, all_of(size), 0.0))
    share(1, 0, slots_c, pair)
    share(1, 1, slots_d, collect(1, 0, slots_c))
    pair = collect(1, 1, slots_d)
    above = jnp.sum(jnp.where(lane == 0, pair, 0.0), axis=1, keepdims=True)
    below = jnp.sum(jnp.where(lane == 1, pair, 0.0), axis=1, keepdims=True)
    change_ref[...] = jnp.broadcast_to(jnp.sqrt(above / (below + 1.0)), (1, slots))


def solution(mesh):
    devices = tuple(mesh.shape[axis] for axis in AXES)

    def on_device(fractions, polarizability, occupancy, pair_mask, perm_field, history):
        tiles = fractions.shape[1:4]
        slots = fractions.shape[4]
        count = tiles[0] * tiles[1] * tiles[2]
        wraps = tuple(n + 2 for n in tiles)
        total_tiles = wraps[0] * wraps[1] * wraps[2]
        past = history.shape[0] - 1
        vmem = pl.BlockSpec(memory_space=pltpu.VMEM)
        f32 = jnp.float32
        groups = [devices[0], devices[1] * devices[2]]
        induced, change = pl.pallas_call(
            functools.partial(kernel, devices),
            out_shape=(
                jax.ShapeDtypeStruct(perm_field.shape, f32),
                jax.ShapeDtypeStruct((1, slots), f32),
            ),
            in_specs=[pl.BlockSpec(memory_space=pltpu.HBM)] * 6,
            out_specs=(vmem, vmem),
            scratch_shapes=[
                pltpu.VMEM(fractions.shape, f32),
                pltpu.VMEM(polarizability.shape, f32),
                pltpu.VMEM(occupancy.shape, jnp.int32),
                pltpu.SMEM(pair_mask.shape, jnp.int32),
                pltpu.VMEM(perm_field.shape, f32),
                pltpu.VMEM(history.shape, f32),
                pltpu.VMEM(wraps + (ROWS, slots), f32),
                pltpu.VMEM(wraps + (past * ROWS, slots), f32),
                pltpu.VMEM(wraps + (ROWS, slots), f32),
                pltpu.VMEM((history.shape[0], count, ROWS, slots), f32),
                pltpu.VMEM((total_tiles, ROWS, slots), f32),
                pltpu.VMEM((total_tiles, 4, slots, slots), f32),
                pltpu.VMEM((total_tiles // 2, 16 * ROWS, 2 * slots), jnp.bfloat16),
                pltpu.VMEM((count, 27, 2 * slots, 2 * slots), jnp.bfloat16),
            ]
            + [pltpu.VMEM((n, 1, slots), f32) for n in groups * 2]
            + [pltpu.VMEM(((total_tiles - count) * past, ROWS, slots), f32)]
            + [
                pltpu.SemaphoreType.DMA((6,)),
                pltpu.SemaphoreType.DMA((2, 2)),
                pltpu.SemaphoreType.DMA((2, 2)),
            ]
            + [pltpu.SemaphoreType.DMA((7,))] * 2,
            compiler_params=pltpu.CompilerParams(
                collective_id=0, has_side_effects=True, vmem_limit_bytes=67043328
            ),
        )(fractions, polarizability, occupancy, pair_mask, perm_field, history)
        return induced, change[0, 0]

    in_specs = (
        P(None, "gx", "gy", "gz", None),
        P("gx", "gy", "gz", None),
        P("gx", "gy", "gz", None),
        P("gx", "gy", "gz", None),
        P(None, "gx", "gy", "gz", None),
        P(None, None, "gx", "gy", "gz", None),
    )
    out_specs = (P(None, "gx", "gy", "gz", None), P())
    return jax.shard_map(
        on_device, mesh=mesh, in_specs=in_specs, out_specs=out_specs, check_vma=False
    )
```

```python
import functools

import jax
import jax.numpy as jnp
from jax import lax
from jax.experimental import pallas as pl
from jax.experimental.pallas import tpu as pltpu
from jax.sharding import PartitionSpec as P

CELL_EDGE = 10.0
SOFTENING = 0.3
THOLE_DAMP = 0.39
RELAXATION = 0.7
LOG2E = 1.4426950408889634
MESH = pl.DeviceIdType.MESH
AXES = ("gx", "gy", "gz")
ROWS = 8
BLOCK = 32
GROUPS = ((0,), (1, 2))


def halo_moves(tiles):
    options = []
    for n in tiles:
        options.append([(0, 0, n, 0), (1, n - 1, 1, n + 1), (-1, 0, 1, n)])
    return [
        (a, b, c) for a in options[0] for b in options[1] for c in options[2] if (a[0], b[0], c[0]) != (0, 0, 0)
    ]


def solve_fit(total, past, lane, pair_lane):
    def pick(a, b):
        index = pair_lane[(min(a, b), max(a, b))]
        return jnp.sum(jnp.where(lane == index, total, 0.0), axis=1, keepdims=True)

    diagonal = [pick(a, a) for a in range(past)]
    trace = diagonal[0]
    for value in diagonal[1:]:
        trace = trace + value
    ridge = 0.001 * trace / past + 1.0
    lower, inverse = {}, []
    for j in range(past):
        pivot = diagonal[j] + ridge
        for m in range(j):
            pivot = pivot - lower[j, m] * lower[j, m]
        inverse.append(lax.rsqrt(pivot))
        for i in range(j + 1, past):
            value = pick(i, j)
            for m in range(j):
                value = value - lower[i, m] * lower[j, m]
            lower[i, j] = value * inverse[j]
    forward = []
    for i in range(past):
        value = pick(i, past)
        for m in range(i):
            value = value - lower[i, m] * forward[m]
        forward.append(value * inverse[i])
    coeffs = [None] * past
    for i in reversed(range(past)):
        value = forward[i]
        for m in range(i + 1, past):
            value = value - lower[m, i] * coeffs[m]
        coeffs[i] = value * inverse[i]
    return coeffs


def kernel(
    devices,
    frac_in, pol_in, occ_in, mask_in, perm_in, hist_in,
    out_ref, change_ref,
    frac_ref, pol_ref, occ_ref, mask_ref, perm_ref, hist_ref,
    geom, held_past, held_two, past_sets, spots, columns, features, weights,
    slots_a, slots_b, slots_c, slots_d, measure,
    load_sem, send_all, recv_all, send_near, recv_near,
):
    tiles = tuple(frac_ref.shape[1:4])
    wraps = tuple(n + 2 for n in tiles)
    slots = frac_ref.shape[4]
    steps = hist_ref.shape[0]
    rows = hist_ref.shape[1]
    past = steps - 1
    at = [lax.axis_index(axis) for axis in AXES]
    moves = halo_moves(tiles)
    lane = lax.broadcasted_iota(jnp.int32, (1, slots), 1)

    loads = [
        pltpu.make_async_copy(source, target, load_sem.at[number])
        for number, (source, target) in enumerate(
            (
                (hist_in, hist_ref), (occ_in, occ_ref), (frac_in, frac_ref),
                (pol_in, pol_ref), (perm_in, perm_ref), (mask_in, mask_ref),
            )
        )
    ]
    for load in loads:
        load.start()

    def size_of(axes):
        total = 1
        for axis in axes:
            total *= devices[axis]
        return total

    def shifted(shift):
        places = []
        for axis in range(3):
            place = at[axis] + shift[axis]
            places.append(jnp.where(place >= devices[axis], place - devices[axis], place))
        return tuple(places)

    def hops(shift):
        return sum(min(part, n - part) for part, n in zip(shift, devices))

    def shifts_of(axes):
        spans = [range(devices[axis]) if axis in axes else range(1) for axis in range(3)]
        every = [(x, y, z) for x in spans[0] for y in spans[1] for z in spans[2] if (x, y, z) != (0, 0, 0)]
        return sorted(every, key=lambda shift: -hops(shift))

    def rank_in(axes):
        rank = 0
        for axis in axes:
            rank = rank * devices[axis] + at[axis]
        return rank

    near = [tuple((move[axis][0] + devices[axis]) % devices[axis] for axis in range(3)) for move in moves]
    greeted = sorted(
        dict.fromkeys([shift for axes in GROUPS for shift in shifts_of(axes)] + near), key=lambda shift: -hops(shift)
    )
    inward = 1 - 2 * lax.bitwise_and(at[0], 1)

    barrier = pltpu.get_barrier_semaphore()
    for shift in greeted:
        pl.semaphore_signal(barrier, inc=1, device_id=shifted(shift), device_id_type=MESH)
    for load in loads:
        load.wait()

    def share(index, stage, held, value):
        axes = GROUPS[stage]
        rank = rank_in(axes)
        held[pl.ds(rank, 1)] = value.reshape(1, 1, slots)
        for shift in shifts_of(axes):
            pltpu.make_async_remote_copy(
                src_ref=held.at[pl.ds(rank, 1)],
                dst_ref=held.at[pl.ds(rank, 1)],
                send_sem=send_all.at[index, stage],
                recv_sem=recv_all.at[index, stage],
                device_id=shifted(shift),
                device_id_type=MESH,
            ).start()

    def collect(index, stage, held):
        others = size_of(GROUPS[stage]) - 1
        whole = pltpu.make_async_remote_copy(
            src_ref=held.at[pl.ds(0, others)],
            dst_ref=held.at[pl.ds(0, others)],
            send_sem=send_all.at[index, stage],
            recv_sem=recv_all.at[index, stage],
            device_id=shifted((0, 0, 1)),
            device_id_type=MESH,
        )
        whole.wait_send()
        whole.wait_recv()
        return jnp.sum(held[...], axis=0)

    def halo(held, send, recv, crossed, on_chip=None):
        for move, shift in zip(moves, near):
            if sum(part[0] != 0 for part in move) not in crossed:
                continue
            number = 0
            if on_chip is not None and move[0][0] != 0:
                number = jnp.where(inward == move[0][0], on_chip, 0)
            source = tuple(pl.ds(part[1], part[2]) for part in move)
            place = tuple(pl.ds(part[3], part[2]) for part in move)
            pltpu.make_async_remote_copy(
                src_ref=held.at[source],
                dst_ref=held.at[place],
                send_sem=send.at[number],
                recv_sem=recv.at[number],
                device_id=shifted(shift),
                device_id_type=MESH,
            ).start()

    def tiles_of(crossed):
        return sum(
            move[0][2] * move[1][2] * move[2][2]
            for move in moves
            if sum(part[0] != 0 for part in move) in crossed
        )

    def halo_wait(held, number, arriving):
        amount = arriving * (held.shape[3] // ROWS)
        whole = pltpu.make_async_remote_copy(
            src_ref=measure.at[pl.ds(0, amount)],
            dst_ref=measure.at[pl.ds(0, amount)],
            send_sem=send_near.at[number],
            recv_sem=recv_near.at[number],
            device_id=shifted(near[0]),
            device_id_type=MESH,
        )
        whole.wait_send()
        whole.wait_recv()

    def row_of(c):
        return 2 * (c % 3) + c // 3

    order = sorted(range(rows), key=row_of)
    places = [(x, y, z) for x in range(tiles[0]) for y in range(tiles[1]) for z in range(tiles[2])]
    count = len(places)
    zero_row = jnp.zeros((1, slots), jnp.float32)
    spare = jnp.zeros((ROWS - rows, slots), jnp.float32)
    scaled = []
    for t, (x, y, z) in enumerate(places):
        full = occ_ref[x, y, z, :].reshape(1, slots).astype(jnp.float32)
        pol = pol_ref[x, y, z, :].reshape(1, slots)
        scaled.append(RELAXATION * full * pol)
        parts = []
        for c in range(3):
            parts += [frac_ref[c, x, y, z, :].reshape(1, slots) * CELL_EDGE] * 2
        geom[x, y, z] = jnp.concatenate(parts + [lax.rsqrt(pol), zero_row], axis=0)
        for h in range(steps):
            moment = jnp.concatenate(
                [hist_ref[h, c, x, y, z, :].reshape(1, slots) for c in order] + [spare], axis=0
            ) * full
            past_sets[h, t] = moment
            if h > 0:
                held_past[x, y, z, pl.ds(ROWS * (h - 1), ROWS), :] = moment
    pair_lane = {}
    gram = zero_row
    for a in range(steps):
        for b in range(a, steps):
            product = past_sets[a, 0] * past_sets[b, 0]
            for t in range(1, count):
                product = product + past_sets[a, t] * past_sets[b, t]
            value = jnp.sum(jnp.sum(product, axis=0, keepdims=True), axis=1, keepdims=True)
            pair_lane[(a, b)] = len(pair_lane)
            gram = jnp.where(lane == pair_lane[(a, b)], value, gram)

    row = lax.broadcasted_iota(jnp.int32, (ROWS, slots), 0)
    wide_row = lax.broadcasted_iota(jnp.int32, (ROWS, 2 * slots), 0)

    square_row = lax.broadcasted_iota(jnp.int32, (slots, slots), 0)
    square_lane = lax.broadcasted_iota(jnp.int32, (slots, slots), 1)

    def flat_of(place):
        return (place[0] * wraps[1] + place[1]) * wraps[2] + place[2]

    def wrap(value, size):
        return jnp.where(value < 0, value + size, value)

    def rounded(value):
        return value.astype(jnp.bfloat16).astype(jnp.float32)

    piece_row = lax.broadcasted_iota(jnp.int32, (4 * ROWS, 4 * slots), 0)
    piece_lane = lax.broadcasted_iota(jnp.int32, (4 * ROWS, 4 * slots), 1)
    chosen_rows = jnp.where(
        jnp.logical_and(
            lax.bitwise_and(piece_row, ROWS - 1) == 2 * lax.shift_right_logical(piece_lane, 7), piece_row < 3 * ROWS
        ),
        1.0,
        0.0,
    ).astype(jnp.bfloat16)

    def prepare(place):
        flat = flat_of(place)
        tile = geom[place[0], place[1], place[2]]
        moved = []
        for axis in range(3):
            number = jnp.where(place[axis] == wraps[axis] - 1, -1, place[axis])
            moved.append(CELL_EDGE * (number.astype(jnp.float32) - 0.5 * tiles[axis]))
        offset = jnp.where(row < 2, moved[0], jnp.where(row < 4, moved[1], jnp.where(row < 6, moved[2], 0.0)))
        tile = tile + offset
        spots[flat] = tile
        middle = tile - rounded(tile)
        last = middle - rounded(middle)
        upright = jnp.concatenate([tile, middle, last, jnp.zeros_like(tile)], axis=0).T
        spread = jnp.dot(upright.astype(jnp.bfloat16), chosen_rows, preferred_element_type=jnp.float32)
        for c in range(4):
            columns[flat, c] = spread[:, c * slots : (c + 1) * slots]

    def split(t):
        return lax.shift_right_logical(t, 1), lax.bitwise_and(t, 1)

    def pair_weights(t, along, itself):
        first_y, first_z = split(t)
        base = (jnp.int32(0), first_y, first_z)
        place = tuple(wrap(base[i] + along[i], wraps[i]) for i in range(3))
        k = 9 * (along[0] + 1) + 3 * (along[1] + 1) + along[2] + 1
        source = flat_of(place)
        own = flat_of(base)
        here = [spots[own, pl.ds(2 * c, 1), :] for c in range(4)]
        allowed = mask_ref[0, first_y, first_z, k].astype(jnp.float32)
        damp = here[3] * (-THOLE_DAMP * allowed)
        for first in range(0, slots, BLOCK):
            part = pl.ds(first, BLOCK)
            dx = columns[source, 0, part, :] - here[0]
            dy = columns[source, 1, part, :] - here[1]
            dz = columns[source, 2, part, :] - here[2]
            square = dx * dx + dy * dy + (dz * dz + SOFTENING)
            root = lax.rsqrt(square)
            root_two = root * root
            cube = root_two * root
            arg = (square * square) * root * (damp * columns[source, 3, part, :])
            fade = jnp.exp2(arg * LOG2E)
            three = 1.0 - fade
            five = three + arg * fade
            radial, direct = five * cube * root_two, three * cube
            if itself:
                apart = square_row[first : first + BLOCK] != square_lane[first : first + BLOCK]
                radial, direct = jnp.where(apart, radial, 0.0), jnp.where(apart, direct, 0.0)
            both = jnp.concatenate([radial, direct], axis=1)
            high = both.astype(jnp.bfloat16)
            weights[t, k, part, :] = high
            weights[t, k, pl.ds(slots + first, BLOCK), :] = (both - high.astype(jnp.float32)).astype(jnp.bfloat16)

    def outward(t):
        first_y, first_z = split(t)
        return 2 * first_y - 1, 2 * first_z - 1

    def weigh(choose):
        def one(t, carry):
            for along in choose(*outward(t)):
                pair_weights(t, along, all(isinstance(part, int) and part == 0 for part in along))
            return carry

        lax.fori_loop(0, count, one, 0)

    def distance(place):
        return sum(part >= n for part, n in zip(place, tiles))

    def prepare_at(crossed, along_x=(0, 1, 2)):
        for x in along_x:
            for y in range(wraps[1]):
                for z in range(wraps[2]):
                    if distance((x, y, z)) == crossed:
                        prepare((jnp.int32(x), jnp.int32(y), jnp.int32(z)))

    def prepare_side(side):
        x = jnp.where(side < 0, wraps[0] - 1, tiles[0])
        for y in range(tiles[1]):
            for z in range(tiles[2]):
                prepare((x, jnp.int32(y), jnp.int32(z)))

    def across(side, y, z):
        return tuple((side, -y * b, -z * c) for b in (0, 1) for c in (0, 1))

    prepare_at(0)
    pl.semaphore_wait(barrier, len(greeted))
    share(0, 0, slots_a, gram)
    def from_sem(first):
        return send_near.at[pl.ds(first, 8 - first)], recv_near.at[pl.ds(first, 8 - first)]

    halo(geom, *from_sem(0), (1,), on_chip=7)
    halo(geom, *from_sem(1), (2,))
    halo(geom, *from_sem(2), (3,))
    everywhere = (1, 2, 3)
    halo(held_past, *from_sem(3), everywhere)
    weigh(lambda y, z: ((0, 0, 0), (0, 0, -z), (0, -y, 0), (0, -y, -z)))
    on_chip_tiles = tiles[1] * tiles[2]
    halo_wait(geom, 7, on_chip_tiles)
    prepare_side(inward)
    weigh(lambda y, z: across(inward, y, z))
    halo_wait(geom, 0, tiles_of((1,)) - on_chip_tiles)
    prepare_side(-inward)
    prepare_at(1, (0,))
    weigh(lambda y, z: ((0, y, 0), (0, y, -z), (0, 0, z), (0, -y, z)))
    share(0, 1, slots_b, collect(0, 0, slots_a))
    weigh(lambda y, z: across(-inward, y, z))
    halo_wait(geom, 1, tiles_of((2,)))
    prepare_at(2)
    weigh(
        lambda y, z: tuple((x,) + side for x in (-1, 1) for side in ((y, 0), (y, -z), (0, z), (-y, z)))
        + ((0, y, z),)
    )
    halo_wait(geom, 2, tiles_of((3,)))
    prepare_at(3)
    weigh(lambda y, z: ((-1, y, z), (1, y, z)))

    def cycle(value):
        value = value + pltpu.roll(value, 4, 0)
        return value + pltpu.roll(value, 2, 0)

    def set_features(pair, moment):
        twice = [2 * pair, 2 * pair + 1]
        spot = jnp.concatenate([spots[flat] for flat in twice], axis=1)
        spot = jnp.where(wide_row < rows, spot, 0.0)
        by = [
            jnp.concatenate([spots[flat, pl.ds(2 * c, 1), :] for flat in twice], axis=1) * moment
            for c in range(3)
        ]
        first = jnp.concatenate([moment, by[0]], axis=0)
        second = jnp.concatenate(by[1:], axis=0)
        third = cycle(spot * moment) * spot
        middle = third - rounded(third)
        last = middle - rounded(middle)
        blocks = []
        for piece in range(3):
            blocks += [first, second]
            if piece < 2:
                first = first - rounded(first)
                second = second - rounded(second)
        blocks.append(jnp.concatenate([third, middle], axis=0))
        blocks.append(jnp.concatenate([last, jnp.zeros_like(last)], axis=0))
        for number, value in enumerate(blocks):
            features[pair, pl.ds(2 * ROWS * number, 2 * ROWS), :] = value.astype(jnp.bfloat16)

    def along_of(k):
        return (k // 9 - 1, k // 3 % 3 - 1, k % 3 - 1)

    def target_of(place, k):
        along = along_of(k)
        return tuple((place[i] + along[i] + wraps[i]) % wraps[i] for i in range(3))

    def partial_sums(t, chosen):
        acc = None
        for k in range(27):
            place = target_of(places[t], k)
            if distance(place) in chosen:
                flat = flat_of(place)
                side = features[flat // 2, :, pl.ds(flat % 2 * slots, slots)]
                part = jnp.dot(
                    jnp.concatenate([side, side], axis=1), weights[t, k], preferred_element_type=jnp.float32
                )
                acc = part if acc is None else acc + part
        group = [acc[ROWS * g : ROWS * (g + 1)] for g in range(2 * ROWS)]
        sums = [(group[8 + g] + group[4 + g] + group[g])[:, 0:slots] for g in range(4)]
        sums.append((group[14] + group[13] + group[12])[:, 0:slots])
        sums.append((group[8] + group[4] + group[0])[:, slots : 2 * slots])
        return sums

    def field_of(t, sums):
        plain, by_x, by_y, by_z, whole, direct = sums
        spot = jnp.where(row < rows, spots[flat_of(places[t])], 0.0)
        mine = [cycle(spot * value) for value in (by_x, by_y, by_z)]
        middle = jnp.where(row < 2, by_x, jnp.where(row < 4, by_y, by_z))
        drawn = jnp.where(row < 2, mine[0], jnp.where(row < 4, mine[1], mine[2]))
        radial = whole - drawn + spot * cycle(spot * plain - middle)
        return jnp.where(row < rows, 3.0 * radial - direct, 0.0)

    fixed = [
        jnp.concatenate([perm_ref[c, x, y, z, :].reshape(1, slots) for c in order] + [spare], axis=0)
        for (x, y, z) in places
    ]
    halo_wait(held_past, 3, tiles_of(everywhere))
    total = collect(0, 1, slots_b)
    coeffs = [jnp.broadcast_to(value, (ROWS, slots)) for value in solve_fit(total, past, lane, pair_lane)]

    def predicted(x, y, z):
        value = coeffs[0] * held_past[x, y, z, pl.ds(0, ROWS), :]
        for h in range(1, past):
            value = value + coeffs[h] * held_past[x, y, z, pl.ds(ROWS * h, ROWS), :]
        return value

    pairs = [(x, y, z) for x in range(wraps[0]) for y in range(wraps[1]) for z in range(0, wraps[2], 2)]
    for x, y, z in pairs:
        set_features(
            flat_of((x, y, z)) // 2, jnp.concatenate([predicted(x, y, z), predicted(x, y, z + 1)], axis=1)
        )
    ones = []
    for t, (x, y, z) in enumerate(places):
        field = field_of(t, partial_sums(t, (0, 1, 2, 3)))
        value = (1.0 - RELAXATION) * predicted(x, y, z) + scaled[t] * (fixed[t] + field)
        held_two[x, y, z] = value
        ones.append(value)
    for crossed in (3, 2, 1):
        halo(held_two, *from_sem(3 + crossed), (crossed,))
    sums = [None] * count
    for near_by in ((0,), (1,), (2,), (3,)):
        if near_by != (0,):
            halo_wait(held_two, 3 + near_by[0], tiles_of(near_by))
        for x, y, z in pairs:
            if distance((x, y, z)) in near_by:
                set_features(
                    flat_of((x, y, z)) // 2,
                    jnp.concatenate([held_two[x, y, z], held_two[x, y, z + 1]], axis=1),
                )
        for t in range(count):
            found = partial_sums(t, near_by)
            sums[t] = found if sums[t] is None else [a + b for a, b in zip(sums[t], found)]
    field = [field_of(t, sums[t]) for t in range(count)]
    changed = jnp.zeros((ROWS, slots), jnp.float32)
    size = jnp.zeros((ROWS, slots), jnp.float32)
    for t, (x, y, z) in enumerate(places):
        before = ones[t]
        after = (1.0 - RELAXATION) * before + scaled[t] * (fixed[t] + field[t])
        for c in range(rows):
            out_ref[c, x, y, z, :] = after[row_of(c)]
        changed = changed + (after - before) * (after - before)
        size = size + after * after

    def all_of(value):
        return jnp.sum(jnp.sum(value, axis=0, keepdims=True), axis=1, keepdims=True)

    pair = jnp.where(lane == 0, all_of(changed), jnp.where(lane == 1, all_of(size), 0.0))
    share(1, 0, slots_c, pair)
    share(1, 1, slots_d, collect(1, 0, slots_c))
    pair = collect(1, 1, slots_d)
    above = jnp.sum(jnp.where(lane == 0, pair, 0.0), axis=1, keepdims=True)
    below = jnp.sum(jnp.where(lane == 1, pair, 0.0), axis=1, keepdims=True)
    change_ref[...] = jnp.broadcast_to(jnp.sqrt(above / (below + 1.0)), (1, slots))


def solution(mesh):
    devices = tuple(mesh.shape[axis] for axis in AXES)

    def on_device(fractions, polarizability, occupancy, pair_mask, perm_field, history):
        tiles = fractions.shape[1:4]
        slots = fractions.shape[4]
        count = tiles[0] * tiles[1] * tiles[2]
        wraps = tuple(n + 2 for n in tiles)
        total_tiles = wraps[0] * wraps[1] * wraps[2]
        past = history.shape[0] - 1
        vmem = pl.BlockSpec(memory_space=pltpu.VMEM)
        f32 = jnp.float32
        groups = [devices[0], devices[1] * devices[2]]
        induced, change = pl.pallas_call(
            functools.partial(kernel, devices),
            out_shape=(
                jax.ShapeDtypeStruct(perm_field.shape, f32),
                jax.ShapeDtypeStruct((1, slots), f32),
            ),
            in_specs=[pl.BlockSpec(memory_space=pltpu.HBM)] * 6,
            out_specs=(vmem, vmem),
            scratch_shapes=[
                pltpu.VMEM(fractions.shape, f32),
                pltpu.VMEM(polarizability.shape, f32),
                pltpu.VMEM(occupancy.shape, jnp.int32),
                pltpu.SMEM(pair_mask.shape, jnp.int32),
                pltpu.VMEM(perm_field.shape, f32),
                pltpu.VMEM(history.shape, f32),
                pltpu.VMEM(wraps + (ROWS, slots), f32),
                pltpu.VMEM(wraps + (past * ROWS, slots), f32),
                pltpu.VMEM(wraps + (ROWS, slots), f32),
                pltpu.VMEM((history.shape[0], count, ROWS, slots), f32),
                pltpu.VMEM((total_tiles, ROWS, slots), f32),
                pltpu.VMEM((total_tiles, 4, slots, slots), f32),
                pltpu.VMEM((total_tiles // 2, 16 * ROWS, 2 * slots), jnp.bfloat16),
                pltpu.VMEM((count, 27, 2 * slots, 2 * slots), jnp.bfloat16),
            ]
            + [pltpu.VMEM((n, 1, slots), f32) for n in groups * 2]
            + [pltpu.VMEM(((total_tiles - count) * past, ROWS, slots), f32)]
            + [
                pltpu.SemaphoreType.DMA((6,)),
                pltpu.SemaphoreType.DMA((2, 2)),
                pltpu.SemaphoreType.DMA((2, 2)),
            ]
            + [pltpu.SemaphoreType.DMA((8,))] * 2,
            compiler_params=pltpu.CompilerParams(
                collective_id=0, has_side_effects=True, vmem_limit_bytes=67043328
            ),
        )(fractions, polarizability, occupancy, pair_mask, perm_field, history)
        return induced, change[0, 0]

    in_specs = (
        P(None, "gx", "gy", "gz", None),
        P("gx", "gy", "gz", None),
        P("gx", "gy", "gz", None),
        P("gx", "gy", "gz", None),
        P(None, "gx", "gy", "gz", None),
        P(None, None, "gx", "gy", "gz", None),
    )
    out_specs = (P(None, "gx", "gy", "gz", None), P())
    return jax.shard_map(
        on_device, mesh=mesh, in_specs=in_specs, out_specs=out_specs, check_vma=False
    )
```

```python
import functools

import jax
import jax.numpy as jnp
from jax import lax
from jax.experimental import pallas as pl
from jax.experimental.pallas import tpu as pltpu
from jax.sharding import PartitionSpec as P

CELL_EDGE = 10.0
SOFTENING = 0.3
THOLE_DAMP = 0.39
RELAXATION = 0.7
LOG2E = 1.4426950408889634
MESH = pl.DeviceIdType.MESH
AXES = ("gx", "gy", "gz")
ROWS = 8
BLOCK = 32
GROUPS = ((0,), (1, 2))


def halo_moves(tiles):
    options = []
    for n in tiles:
        options.append([(0, 0, n, 0), (1, n - 1, 1, n + 1), (-1, 0, 1, n)])
    return [
        (a, b, c) for a in options[0] for b in options[1] for c in options[2] if (a[0], b[0], c[0]) != (0, 0, 0)
    ]


def solve_fit(total, past, lane, pair_lane):
    def pick(a, b):
        index = pair_lane[(min(a, b), max(a, b))]
        return jnp.sum(jnp.where(lane == index, total, 0.0), axis=1, keepdims=True)

    diagonal = [pick(a, a) for a in range(past)]
    trace = diagonal[0]
    for value in diagonal[1:]:
        trace = trace + value
    ridge = 0.001 * trace / past + 1.0
    lower, inverse = {}, []
    for j in range(past):
        pivot = diagonal[j] + ridge
        for m in range(j):
            pivot = pivot - lower[j, m] * lower[j, m]
        inverse.append(lax.rsqrt(pivot))
        for i in range(j + 1, past):
            value = pick(i, j)
            for m in range(j):
                value = value - lower[i, m] * lower[j, m]
            lower[i, j] = value * inverse[j]
    forward = []
    for i in range(past):
        value = pick(i, past)
        for m in range(i):
            value = value - lower[i, m] * forward[m]
        forward.append(value * inverse[i])
    coeffs = [None] * past
    for i in reversed(range(past)):
        value = forward[i]
        for m in range(i + 1, past):
            value = value - lower[m, i] * coeffs[m]
        coeffs[i] = value * inverse[i]
    return coeffs


def kernel(
    devices,
    frac_in, pol_in, occ_in, mask_in, perm_in, hist_in,
    out_ref, change_ref,
    frac_ref, pol_ref, occ_ref, mask_ref, perm_ref, hist_ref,
    geom, held_past, held_two, past_sets, spots, columns, features, weights,
    slots_a, slots_b, slots_c, slots_d, measure,
    load_sem, send_all, recv_all, send_near, recv_near,
):
    tiles = tuple(frac_ref.shape[1:4])
    wraps = tuple(n + 2 for n in tiles)
    slots = frac_ref.shape[4]
    steps = hist_ref.shape[0]
    rows = hist_ref.shape[1]
    past = steps - 1
    at = [lax.axis_index(axis) for axis in AXES]
    moves = halo_moves(tiles)
    lane = lax.broadcasted_iota(jnp.int32, (1, slots), 1)

    loads = [
        pltpu.make_async_copy(source, target, load_sem.at[number])
        for number, (source, target) in enumerate(
            (
                (hist_in, hist_ref), (occ_in, occ_ref), (frac_in, frac_ref),
                (pol_in, pol_ref), (perm_in, perm_ref), (mask_in, mask_ref),
            )
        )
    ]
    for load in loads:
        load.start()

    def size_of(axes):
        total = 1
        for axis in axes:
            total *= devices[axis]
        return total

    def shifted(shift):
        places = []
        for axis in range(3):
            place = at[axis] + shift[axis]
            places.append(jnp.where(place >= devices[axis], place - devices[axis], place))
        return tuple(places)

    def hops(shift):
        return sum(min(part, n - part) for part, n in zip(shift, devices))

    def shifts_of(axes):
        spans = [range(devices[axis]) if axis in axes else range(1) for axis in range(3)]
        every = [(x, y, z) for x in spans[0] for y in spans[1] for z in spans[2] if (x, y, z) != (0, 0, 0)]
        return sorted(every, key=lambda shift: -hops(shift))

    def rank_in(axes):
        rank = 0
        for axis in axes:
            rank = rank * devices[axis] + at[axis]
        return rank

    near = [tuple((move[axis][0] + devices[axis]) % devices[axis] for axis in range(3)) for move in moves]
    greeted = sorted(
        dict.fromkeys([shift for axes in GROUPS for shift in shifts_of(axes)] + near), key=lambda shift: -hops(shift)
    )
    inward = 1 - 2 * lax.bitwise_and(at[0], 1)

    barrier = pltpu.get_barrier_semaphore()
    for shift in greeted:
        pl.semaphore_signal(barrier, inc=1, device_id=shifted(shift), device_id_type=MESH)
    for load in loads:
        load.wait()

    def share(index, stage, held, value):
        axes = GROUPS[stage]
        rank = rank_in(axes)
        held[pl.ds(rank, 1)] = value.reshape(1, 1, slots)
        for shift in shifts_of(axes):
            pltpu.make_async_remote_copy(
                src_ref=held.at[pl.ds(rank, 1)],
                dst_ref=held.at[pl.ds(rank, 1)],
                send_sem=send_all.at[index, stage],
                recv_sem=recv_all.at[index, stage],
                device_id=shifted(shift),
                device_id_type=MESH,
            ).start()

    def collect(index, stage, held):
        others = size_of(GROUPS[stage]) - 1
        whole = pltpu.make_async_remote_copy(
            src_ref=held.at[pl.ds(0, others)],
            dst_ref=held.at[pl.ds(0, others)],
            send_sem=send_all.at[index, stage],
            recv_sem=recv_all.at[index, stage],
            device_id=shifted((0, 0, 1)),
            device_id_type=MESH,
        )
        whole.wait_send()
        whole.wait_recv()
        return jnp.sum(held[...], axis=0)

    def halo(held, send, recv, crossed, on_chip=None, sent_rows=None):
        for move, shift in zip(moves, near):
            if sum(part[0] != 0 for part in move) not in crossed:
                continue
            number = 0
            if on_chip is not None and move[0][0] != 0:
                number = jnp.where(inward == move[0][0], on_chip, 0)
            source = tuple(pl.ds(part[1], part[2]) for part in move)
            place = tuple(pl.ds(part[3], part[2]) for part in move)
            if sent_rows is not None:
                source, place = source + (pl.ds(0, sent_rows),), place + (pl.ds(0, sent_rows),)
            pltpu.make_async_remote_copy(
                src_ref=held.at[source],
                dst_ref=held.at[place],
                send_sem=send.at[number],
                recv_sem=recv.at[number],
                device_id=shifted(shift),
                device_id_type=MESH,
            ).start()

    def tiles_of(crossed):
        return sum(
            move[0][2] * move[1][2] * move[2][2]
            for move in moves
            if sum(part[0] != 0 for part in move) in crossed
        )

    def halo_wait(sent_rows, number, arriving):
        amount = arriving * sent_rows // ROWS
        whole = pltpu.make_async_remote_copy(
            src_ref=measure.at[pl.ds(0, amount)],
            dst_ref=measure.at[pl.ds(0, amount)],
            send_sem=send_near.at[number],
            recv_sem=recv_near.at[number],
            device_id=shifted(near[0]),
            device_id_type=MESH,
        )
        whole.wait_send()
        whole.wait_recv()

    def row_of(c):
        return 2 * (c % 3) + c // 3

    order = sorted(range(rows), key=row_of)
    places = [(x, y, z) for x in range(tiles[0]) for y in range(tiles[1]) for z in range(tiles[2])]
    count = len(places)
    zero_row = jnp.zeros((1, slots), jnp.float32)
    spare = jnp.zeros((ROWS - rows, slots), jnp.float32)
    scaled = []
    for t, (x, y, z) in enumerate(places):
        full = occ_ref[x, y, z, :].reshape(1, slots).astype(jnp.float32)
        pol = pol_ref[x, y, z, :].reshape(1, slots)
        scaled.append(RELAXATION * full * pol)
        parts = []
        for c in range(3):
            parts += [frac_ref[c, x, y, z, :].reshape(1, slots) * CELL_EDGE] * 2
        geom[x, y, z] = jnp.concatenate(parts + [lax.rsqrt(pol), zero_row], axis=0)
        for h in range(steps):
            moment = jnp.concatenate(
                [hist_ref[h, c, x, y, z, :].reshape(1, slots) for c in order] + [spare], axis=0
            ) * full
            past_sets[h, t] = moment
            if h > 0:
                held_past[x, y, z, pl.ds(rows * (h - 1), rows), :] = moment[0:rows]
        held_past[x, y, z, pl.ds(rows * past, ROWS - rows), :] = spare
    pair_lane = {}
    gram = zero_row
    for a in range(steps):
        for b in range(a, steps):
            product = past_sets[a, 0] * past_sets[b, 0]
            for t in range(1, count):
                product = product + past_sets[a, t] * past_sets[b, t]
            value = jnp.sum(jnp.sum(product, axis=0, keepdims=True), axis=1, keepdims=True)
            pair_lane[(a, b)] = len(pair_lane)
            gram = jnp.where(lane == pair_lane[(a, b)], value, gram)

    row = lax.broadcasted_iota(jnp.int32, (ROWS, slots), 0)
    wide_row = lax.broadcasted_iota(jnp.int32, (ROWS, 2 * slots), 0)

    square_row = lax.broadcasted_iota(jnp.int32, (slots, slots), 0)
    square_lane = lax.broadcasted_iota(jnp.int32, (slots, slots), 1)

    def flat_of(place):
        return (place[0] * wraps[1] + place[1]) * wraps[2] + place[2]

    def wrap(value, size):
        return jnp.where(value < 0, value + size, value)

    def rounded(value):
        return value.astype(jnp.bfloat16).astype(jnp.float32)

    piece_row = lax.broadcasted_iota(jnp.int32, (4 * ROWS, 4 * slots), 0)
    piece_lane = lax.broadcasted_iota(jnp.int32, (4 * ROWS, 4 * slots), 1)
    chosen_rows = jnp.where(
        jnp.logical_and(
            lax.bitwise_and(piece_row, ROWS - 1) == 2 * lax.shift_right_logical(piece_lane, 7), piece_row < 3 * ROWS
        ),
        1.0,
        0.0,
    ).astype(jnp.bfloat16)

    def prepare(place):
        flat = flat_of(place)
        tile = geom[place[0], place[1], place[2]]
        moved = []
        for axis in range(3):
            number = jnp.where(place[axis] == wraps[axis] - 1, -1, place[axis])
            moved.append(CELL_EDGE * (number.astype(jnp.float32) - 0.5 * tiles[axis]))
        offset = jnp.where(row < 2, moved[0], jnp.where(row < 4, moved[1], jnp.where(row < 6, moved[2], 0.0)))
        tile = tile + offset
        spots[flat] = tile
        middle = tile - rounded(tile)
        last = middle - rounded(middle)
        upright = jnp.concatenate([tile, middle, last, jnp.zeros_like(tile)], axis=0).T
        spread = jnp.dot(upright.astype(jnp.bfloat16), chosen_rows, preferred_element_type=jnp.float32)
        for c in range(4):
            columns[flat, c] = spread[:, c * slots : (c + 1) * slots]

    def split(t):
        return lax.shift_right_logical(t, 1), lax.bitwise_and(t, 1)

    def pair_weights(t, along, itself):
        first_y, first_z = split(t)
        base = (jnp.int32(0), first_y, first_z)
        place = tuple(wrap(base[i] + along[i], wraps[i]) for i in range(3))
        k = 9 * (along[0] + 1) + 3 * (along[1] + 1) + along[2] + 1
        source = flat_of(place)
        own = flat_of(base)
        here = [spots[own, pl.ds(2 * c, 1), :] for c in range(4)]
        allowed = mask_ref[0, first_y, first_z, k].astype(jnp.float32)
        damp = here[3] * (-THOLE_DAMP * allowed)
        for first in range(0, slots, BLOCK):
            part = pl.ds(first, BLOCK)
            dx = columns[source, 0, part, :] - here[0]
            dy = columns[source, 1, part, :] - here[1]
            dz = columns[source, 2, part, :] - here[2]
            square = dx * dx + dy * dy + (dz * dz + SOFTENING)
            root = lax.rsqrt(square)
            root_two = root * root
            cube = root_two * root
            arg = (square * square) * root * (damp * columns[source, 3, part, :])
            fade = jnp.exp2(arg * LOG2E)
            three = 1.0 - fade
            five = three + arg * fade
            radial, direct = five * cube * root_two, three * cube
            if itself:
                apart = square_row[first : first + BLOCK] != square_lane[first : first + BLOCK]
                radial, direct = jnp.where(apart, radial, 0.0), jnp.where(apart, direct, 0.0)
            both = jnp.concatenate([radial, direct], axis=1)
            high = both.astype(jnp.bfloat16)
            weights[t, k, part, :] = high
            weights[t, k, pl.ds(slots + first, BLOCK), :] = (both - high.astype(jnp.float32)).astype(jnp.bfloat16)

    def outward(t):
        first_y, first_z = split(t)
        return 2 * first_y - 1, 2 * first_z - 1

    def weigh(choose):
        def one(t, carry):
            for along in choose(*outward(t)):
                pair_weights(t, along, all(isinstance(part, int) and part == 0 for part in along))
            return carry

        lax.fori_loop(0, count, one, 0)

    def distance(place):
        return sum(part >= n for part, n in zip(place, tiles))

    def prepare_at(crossed, along_x=(0, 1, 2)):
        for x in along_x:
            for y in range(wraps[1]):
                for z in range(wraps[2]):
                    if distance((x, y, z)) == crossed:
                        prepare((jnp.int32(x), jnp.int32(y), jnp.int32(z)))

    def prepare_side(side):
        x = jnp.where(side < 0, wraps[0] - 1, tiles[0])
        for y in range(tiles[1]):
            for z in range(tiles[2]):
                prepare((x, jnp.int32(y), jnp.int32(z)))

    def across(side, y, z):
        return tuple((side, -y * b, -z * c) for b in (0, 1) for c in (0, 1))

    prepare_at(0)
    pl.semaphore_wait(barrier, len(greeted))
    share(0, 0, slots_a, gram)
    def from_sem(first):
        return send_near.at[pl.ds(first, 8 - first)], recv_near.at[pl.ds(first, 8 - first)]

    halo(geom, *from_sem(0), (1,), on_chip=7)
    halo(geom, *from_sem(1), (2,))
    halo(geom, *from_sem(2), (3,))
    everywhere = (1, 2, 3)
    halo(held_past, *from_sem(3), everywhere)
    weigh(lambda y, z: ((0, 0, 0), (0, 0, -z), (0, -y, 0), (0, -y, -z)))
    on_chip_tiles = tiles[1] * tiles[2]
    halo_wait(ROWS, 7, on_chip_tiles)
    prepare_side(inward)
    weigh(lambda y, z: across(inward, y, z))
    halo_wait(ROWS, 0, tiles_of((1,)) - on_chip_tiles)
    prepare_side(-inward)
    prepare_at(1, (0,))
    weigh(lambda y, z: ((0, y, 0), (0, y, -z), (0, 0, z), (0, -y, z)))
    share(0, 1, slots_b, collect(0, 0, slots_a))
    weigh(lambda y, z: across(-inward, y, z))
    halo_wait(ROWS, 1, tiles_of((2,)))
    prepare_at(2)
    weigh(
        lambda y, z: tuple((x,) + side for x in (-1, 1) for side in ((y, 0), (y, -z), (0, z), (-y, z)))
        + ((0, y, z),)
    )
    halo_wait(ROWS, 2, tiles_of((3,)))
    prepare_at(3)
    weigh(lambda y, z: ((-1, y, z), (1, y, z)))

    def cycle(value):
        value = value + pltpu.roll(value, 4, 0)
        return value + pltpu.roll(value, 2, 0)

    def set_features(pair, moment):
        twice = [2 * pair, 2 * pair + 1]
        spot = jnp.concatenate([spots[flat] for flat in twice], axis=1)
        spot = jnp.where(wide_row < rows, spot, 0.0)
        by = [
            jnp.concatenate([spots[flat, pl.ds(2 * c, 1), :] for flat in twice], axis=1) * moment
            for c in range(3)
        ]
        first = jnp.concatenate([moment, by[0]], axis=0)
        second = jnp.concatenate(by[1:], axis=0)
        third = cycle(spot * moment) * spot
        middle = third - rounded(third)
        last = middle - rounded(middle)
        blocks = []
        for piece in range(3):
            blocks += [first, second]
            if piece < 2:
                first = first - rounded(first)
                second = second - rounded(second)
        blocks.append(jnp.concatenate([third, middle], axis=0))
        blocks.append(jnp.concatenate([last, jnp.zeros_like(last)], axis=0))
        for number, value in enumerate(blocks):
            features[pair, pl.ds(2 * ROWS * number, 2 * ROWS), :] = value.astype(jnp.bfloat16)

    def along_of(k):
        return (k // 9 - 1, k // 3 % 3 - 1, k % 3 - 1)

    def target_of(place, k):
        along = along_of(k)
        return tuple((place[i] + along[i] + wraps[i]) % wraps[i] for i in range(3))

    def partial_sums(t, chosen):
        acc = None
        for k in range(27):
            place = target_of(places[t], k)
            if distance(place) in chosen:
                flat = flat_of(place)
                side = features[flat // 2, :, pl.ds(flat % 2 * slots, slots)]
                part = jnp.dot(
                    jnp.concatenate([side, side], axis=1), weights[t, k], preferred_element_type=jnp.float32
                )
                acc = part if acc is None else acc + part
        group = [acc[ROWS * g : ROWS * (g + 1)] for g in range(2 * ROWS)]
        sums = [(group[8 + g] + group[4 + g] + group[g])[:, 0:slots] for g in range(4)]
        sums.append((group[14] + group[13] + group[12])[:, 0:slots])
        sums.append((group[8] + group[4] + group[0])[:, slots : 2 * slots])
        return sums

    def field_of(t, sums):
        plain, by_x, by_y, by_z, whole, direct = sums
        spot = jnp.where(row < rows, spots[flat_of(places[t])], 0.0)
        mine = [cycle(spot * value) for value in (by_x, by_y, by_z)]
        middle = jnp.where(row < 2, by_x, jnp.where(row < 4, by_y, by_z))
        drawn = jnp.where(row < 2, mine[0], jnp.where(row < 4, mine[1], mine[2]))
        radial = whole - drawn + spot * cycle(spot * plain - middle)
        return jnp.where(row < rows, 3.0 * radial - direct, 0.0)

    fixed = [
        jnp.concatenate([perm_ref[c, x, y, z, :].reshape(1, slots) for c in order] + [spare], axis=0)
        for (x, y, z) in places
    ]
    halo_wait(4 * ROWS, 3, tiles_of(everywhere))
    total = collect(0, 1, slots_b)
    coeffs = [jnp.broadcast_to(value, (ROWS, slots)) for value in solve_fit(total, past, lane, pair_lane)]

    def predicted(x, y, z):
        value = coeffs[0] * held_past[x, y, z, pl.ds(0, ROWS), :]
        for h in range(1, past):
            value = value + coeffs[h] * held_past[x, y, z, pl.ds(rows * h, ROWS), :]
        return jnp.where(row < rows, value, 0.0)

    pairs = [(x, y, z) for x in range(wraps[0]) for y in range(wraps[1]) for z in range(0, wraps[2], 2)]
    for x, y, z in pairs:
        set_features(
            flat_of((x, y, z)) // 2, jnp.concatenate([predicted(x, y, z), predicted(x, y, z + 1)], axis=1)
        )
    ones = []
    for t, (x, y, z) in enumerate(places):
        field = field_of(t, partial_sums(t, (0, 1, 2, 3)))
        value = (1.0 - RELAXATION) * predicted(x, y, z) + scaled[t] * (fixed[t] + field)
        held_two[x, y, z] = value
        ones.append(value)
    for crossed in (3, 2, 1):
        halo(held_two, *from_sem(3 + crossed), (crossed,), sent_rows=rows)
    sums = [None] * count
    for near_by in ((0,), (1,), (2,), (3,)):
        if near_by != (0,):
            halo_wait(rows, 3 + near_by[0], tiles_of(near_by))
        for x, y, z in pairs:
            if distance((x, y, z)) in near_by:
                set_features(
                    flat_of((x, y, z)) // 2,
                    jnp.where(
                        wide_row < rows,
                        jnp.concatenate([held_two[x, y, z], held_two[x, y, z + 1]], axis=1),
                        0.0,
                    ),
                )
        for t in range(count):
            found = partial_sums(t, near_by)
            sums[t] = found if sums[t] is None else [a + b for a, b in zip(sums[t], found)]
    field = [field_of(t, sums[t]) for t in range(count)]
    changed = jnp.zeros((ROWS, slots), jnp.float32)
    size = jnp.zeros((ROWS, slots), jnp.float32)
    for t, (x, y, z) in enumerate(places):
        before = ones[t]
        after = (1.0 - RELAXATION) * before + scaled[t] * (fixed[t] + field[t])
        for c in range(rows):
            out_ref[c, x, y, z, :] = after[row_of(c)]
        changed = changed + (after - before) * (after - before)
        size = size + after * after

    def all_of(value):
        return jnp.sum(jnp.sum(value, axis=0, keepdims=True), axis=1, keepdims=True)

    pair = jnp.where(lane == 0, all_of(changed), jnp.where(lane == 1, all_of(size), 0.0))
    share(1, 0, slots_c, pair)
    share(1, 1, slots_d, collect(1, 0, slots_c))
    pair = collect(1, 1, slots_d)
    above = jnp.sum(jnp.where(lane == 0, pair, 0.0), axis=1, keepdims=True)
    below = jnp.sum(jnp.where(lane == 1, pair, 0.0), axis=1, keepdims=True)
    change_ref[...] = jnp.broadcast_to(jnp.sqrt(above / (below + 1.0)), (1, slots))


def solution(mesh):
    devices = tuple(mesh.shape[axis] for axis in AXES)

    def on_device(fractions, polarizability, occupancy, pair_mask, perm_field, history):
        tiles = fractions.shape[1:4]
        slots = fractions.shape[4]
        count = tiles[0] * tiles[1] * tiles[2]
        wraps = tuple(n + 2 for n in tiles)
        total_tiles = wraps[0] * wraps[1] * wraps[2]
        past = history.shape[0] - 1
        vmem = pl.BlockSpec(memory_space=pltpu.VMEM)
        f32 = jnp.float32
        groups = [devices[0], devices[1] * devices[2]]
        induced, change = pl.pallas_call(
            functools.partial(kernel, devices),
            out_shape=(
                jax.ShapeDtypeStruct(perm_field.shape, f32),
                jax.ShapeDtypeStruct((1, slots), f32),
            ),
            in_specs=[pl.BlockSpec(memory_space=pltpu.HBM)] * 6,
            out_specs=(vmem, vmem),
            scratch_shapes=[
                pltpu.VMEM(fractions.shape, f32),
                pltpu.VMEM(polarizability.shape, f32),
                pltpu.VMEM(occupancy.shape, jnp.int32),
                pltpu.SMEM(pair_mask.shape, jnp.int32),
                pltpu.VMEM(perm_field.shape, f32),
                pltpu.VMEM(history.shape, f32),
                pltpu.VMEM(wraps + (ROWS, slots), f32),
                pltpu.VMEM(wraps + (4 * ROWS, slots), f32),
                pltpu.VMEM(wraps + (ROWS, slots), f32),
                pltpu.VMEM((history.shape[0], count, ROWS, slots), f32),
                pltpu.VMEM((total_tiles, ROWS, slots), f32),
                pltpu.VMEM((total_tiles, 4, slots, slots), f32),
                pltpu.VMEM((total_tiles // 2, 16 * ROWS, 2 * slots), jnp.bfloat16),
                pltpu.VMEM((count, 27, 2 * slots, 2 * slots), jnp.bfloat16),
            ]
            + [pltpu.VMEM((n, 1, slots), f32) for n in groups * 2]
            + [pltpu.VMEM(((total_tiles - count) * past, ROWS, slots), f32)]
            + [
                pltpu.SemaphoreType.DMA((6,)),
                pltpu.SemaphoreType.DMA((2, 2)),
                pltpu.SemaphoreType.DMA((2, 2)),
            ]
            + [pltpu.SemaphoreType.DMA((8,))] * 2,
            compiler_params=pltpu.CompilerParams(
                collective_id=0, has_side_effects=True, vmem_limit_bytes=67043328
            ),
        )(fractions, polarizability, occupancy, pair_mask, perm_field, history)
        return induced, change[0, 0]

    in_specs = (
        P(None, "gx", "gy", "gz", None),
        P("gx", "gy", "gz", None),
        P("gx", "gy", "gz", None),
        P("gx", "gy", "gz", None),
        P(None, "gx", "gy", "gz", None),
        P(None, None, "gx", "gy", "gz", None),
    )
    out_specs = (P(None, "gx", "gy", "gz", None), P())
    return jax.shard_map(
        on_device, mesh=mesh, in_specs=in_specs, out_specs=out_specs, check_vma=False
    )
```
